128 devices in a mesh: row: 16 (over y, z), col: 8 (over x, core).
Axes of the slice: x: 4, y: 4, z: 4, core: 2. Of those that a mesh axis runs over, the one named last changes fastest.
Arguments:
- conductance: float32 [512, 4096], P('row', 'col'), may hold values from 0.1 to 10
- nodata_mask: int32 [512, 4096], P('row', 'col'), may hold values 0 or 1
- source_index: int32 [16, 16], replicated, may hold values from 0 to 2097151
- source_current: float32 [16, 16], replicated, may hold values from 1 to 10
- ground_index: int32 [16, 16], replicated, may hold values from 0 to 2097151
Outputs:
- voltage: float32 [16, 512, 4096], P(None, 'row', 'col')
The draws below stay inside these ranges and needn't reach their ends.
Inputs may be any that keep to these rules, and one draw needn't show every extreme that they name: `source_index`: each source's row is its index // 4096 and its column its index % 4096; indices may repeat and may name nodata cells. `ground_index`: read as source_index; a ground on a nodata cell still counts.
All inputs are finite; a program needn't handle non-finite values. No bound on the sum of `nodata_mask` on one device may be relied on, other than what follows from the above.
Results may differ from the reference program's by a relative error of at most 0.0003.
Values sent between devices are 32-bit elements; how exact they have to be, the bound alone decides.
A program may use at most 64 MiB of HBM per device.

```python
import math
import jax
import jax.numpy as jnp
from jax import lax

NB = 16
CR = 32
CC = 512
NSRC = 16
NGND = 16
SWEEPS = 5
ITERS = 3
NR = 512
NC = 4096
N_ROW = 16
N_COL = 8


def plant(array, rng, smallest, largest):
    longest = array.shape.index(max(array.shape))
    spots = []
    for shift in (0, 1):
        where = [jax.random.randint(jax.random.fold_in(rng, axis), (), 0, length) for axis, length in enumerate(array.shape)]
        where[longest] = (where[longest] + shift) % array.shape[longest]
        spots.append(tuple(where))
    return array.at[spots[0]].set(smallest).at[spots[1]].set(largest)


def steps_of(rng, dims, split, least, top_value):
    def one(axis_at, parts):
        steps = jax.random.uniform(jax.random.fold_in(jax.random.fold_in(rng, 6), axis_at), (parts,), jnp.float32, least / len(split), top_value / len(split))
        return jnp.repeat(jnp.exp(steps), dims[axis_at] // parts).reshape((-1,) + (1,) * (len(dims) - axis_at - 1))

    gain = one(*split[0])
    for cut in split[1:]:
        gain = gain * one(*cut)
    return gain


def setup_inputs(seed: int = 0) -> dict:
    streams_of = jax.random.split(jax.random.key(seed), 6)
    return {
        "conductance": jnp.clip(jnp.exp(math.log(10.0) - 4.6051702 * jax.random.uniform(streams_of[0], (NR, NC), jnp.float32) ** steps_of(streams_of[0], (NR, NC), ((0, 16), (1, 8)), -0.2, 0.2)), 0.1, 10.0),
        "nodata_mask": plant((jax.random.randint(streams_of[1], (NR, NC), 0, 10) < 9).astype(jnp.int32), jax.random.fold_in(streams_of[1], 1), 0, 1),
        "source_index": plant(jax.random.randint(streams_of[2], (NB, NSRC), 0, NR * NC), jax.random.fold_in(streams_of[2], 1), 0, (NR * NC) - 1).astype(jnp.int32),
        "source_current": jnp.clip(jnp.exp(jax.random.uniform(streams_of[3], (NB, NSRC), jnp.float32, math.log(1.0), math.log(10.0))), 1.0, 10.0),
        "ground_index": plant(jax.random.randint(streams_of[4], (NB, NGND), 0, NR * NC), jax.random.fold_in(streams_of[4], 1), 0, (NR * NC) - 1).astype(jnp.int32),
    }


LEAKAGE = 0.0001
GROUND_CONDUCTANCE = 1.0
RELAXATION = 2.0 / 3.0

def take_east(field):
    return jnp.pad(field[:, 1:], ((0, 0), (0, 1)))

def take_west(field):
    return jnp.pad(field[:, :-1], ((0, 0), (1, 0)))

def take_south(field):
    return jnp.pad(field[1:], ((0, 1), (0, 0)))

def take_north(field):
    return jnp.pad(field[:-1], ((1, 0), (0, 0)))

def block_total(field):
    return field.reshape(N_ROW, CR, N_COL, CC).sum(axis=(1, 3)).reshape(-1)

def spread_blocks(values):
    return jnp.broadcast_to(values.reshape(N_ROW, 1, N_COL, 1), (N_ROW, CR, N_COL, CC)).reshape(NR, NC)

def coarse_solve(factor, rhs):
    forward = lax.linalg.triangular_solve(factor, rhs, left_side=True, lower=True)
    return lax.linalg.triangular_solve(factor, forward, left_side=True, lower=True, transpose_a=True)

def reference(conductance, nodata_mask, source_index, source_current, ground_index):
    present = nodata_mask.astype(jnp.float32)
    masked = conductance * present
    east_edge = 0.5 * present * take_east(present) * (masked + take_east(masked))
    south_edge = 0.5 * present * take_south(present) * (masked + take_south(masked))
    west_edge = take_west(east_edge)
    north_edge = take_north(south_edge)
    base = east_edge + west_edge + south_edge + north_edge + LEAKAGE
    east_cross = east_edge[:, CC - 1::CC].reshape(N_ROW, CR, N_COL).sum(axis=1)
    south_cross = south_edge[CR - 1::CR, :].reshape(N_ROW, N_COL, CC).sum(axis=2)
    east_flat = east_cross.reshape(-1)
    south_flat = south_cross.reshape(-1)
    east_west = jnp.pad(east_cross[:, :-1], ((0, 0), (1, 0))).reshape(-1)
    south_north = jnp.pad(south_cross[:-1], ((1, 0), (0, 0))).reshape(-1)
    coupling = jnp.diag(east_flat[:-1], 1) + jnp.diag(east_flat[:-1], -1) + jnp.diag(south_flat[:-N_COL], N_COL) + jnp.diag(south_flat[:-N_COL], -N_COL)

    def solve_one(inputs):
        sources, currents, grounds = inputs
        shunt = jnp.zeros((NR * NC,), jnp.float32).at[grounds].add(GROUND_CONDUCTANCE).reshape(NR, NC)
        inflow = jnp.zeros((NR * NC,), jnp.float32).at[sources].add(currents).reshape(NR, NC) * present
        diagonal = base + shunt
        inverse = 1.0 / diagonal

        def operate(field):
            return diagonal * field - east_edge * take_east(field) - west_edge * take_west(field) - south_edge * take_south(field) - north_edge * take_north(field)
        shunt_total = LEAKAGE * CR * CC + block_total(shunt)
        degree = shunt_total + east_flat + east_west + south_flat + south_north
        factor = jnp.linalg.cholesky(jnp.diag(degree) - coupling)

        def precondition(residual):
            smooth = RELAXATION * inverse * residual
            for sweep_step in range(SWEEPS - 1):
                smooth = smooth + RELAXATION * inverse * (residual - operate(smooth))
            solved = coarse_solve(factor, block_total(residual)[:, None])[:, 0]
            return smooth + spread_blocks(solved)
        voltage = jnp.zeros((NR, NC), jnp.float32)
        residual = inflow
        precond = precondition(residual)
        direction = precond
        energy = jnp.sum(residual * precond)
        for iteration_step in range(ITERS):
            image = operate(direction)
            alpha = energy / jnp.sum(direction * image)
            voltage = voltage + alpha * direction
            if iteration_step + 1 < ITERS:
                residual = residual - alpha * image
                precond = precondition(residual)
                energy_next = jnp.sum(residual * precond)
                direction = precond + energy_next / energy * direction
                energy = energy_next
        return voltage
    return lax.map(solve_one, (source_index, source_current, ground_index))
```

```python
import jax
import jax.numpy as jnp
from jax import lax
from jax.experimental import pallas as pl
from jax.experimental.pallas import tpu as pltpu
from jax.sharding import PartitionSpec as P

LEAKAGE = 0.0001
RELAXATION = 2.0 / 3.0
NB = 16
CR = 32
CC = 512
N_ROW = 16
N_COL = 8
NC = N_COL * CC
MARGIN = 16
WR = CR + 2 * MARGIN
WC = CC + 128
F32 = jnp.float32
BF16 = jnp.bfloat16
MESH = pl.DeviceIdType.MESH
NT = (((1,), (1,)), ((), ()))


def iota(shape, dim):
    return lax.broadcasted_iota(jnp.int32, shape, dim)


def roll(x, shift):
    return pltpu.roll(x, shift % x.shape[-1], x.ndim - 1)


def flat_row(x):
    pick = (iota((16, 256), 1) % 16 == iota((16, 256), 0)).astype(F32)
    tiled = jnp.dot(x, pick, precision=lax.Precision.HIGHEST, preferred_element_type=F32)
    own = iota((16, 256), 1) // 16 == iota((16, 256), 0)
    return jnp.sum(jnp.where(own, tiled, 0.0), axis=0, keepdims=True)


def mat_mat(a, b):
    out = []
    for j in range(8):
        total = a[0] * b[j][0:1, :]
        for k in range(1, 8):
            total = total + a[k] * b[j][k : k + 1, :]
        out.append(total)
    return out


def mat_vec(a, f):
    parts = [a[k] * f[k : k + 1, :] for k in range(8)]
    while len(parts) > 1:
        parts = [parts[i] + parts[i + 1] for i in range(0, len(parts), 2)]
    return parts[0]


def mat_inv(t):
    t = list(t)
    sub = iota((8, 256), 0)
    for k in range(8):
        pivot = 1.0 / t[k][k : k + 1, :]
        column = t[k]
        at_k = sub == k
        for j in range(8):
            if j != k:
                row = t[j][k : k + 1, :] * pivot
                t[j] = jnp.where(at_k, row, t[j] - column * row)
        t[k] = jnp.where(at_k, pivot, -column * pivot)
    return t


def body(
    cond, mask, sidx, scur, gidx, out,
    mwin, side_r, side_l, diag, hsrc, winv, e_east, e_south, kappa,
    s_a, s_b, v0, v1, w0, w1, lhs_g, lhs_s, cfac, clow, cup, mrow,
    ga0, gb0, ga1, gb1, ga2, gb2, ga3, gb3,
    halo_send, halo_recv, ga_send, ga_recv, gb_send, gb_recv,
):
    rho = lax.axis_index("row")
    col = lax.axis_index("col")
    gas = (ga0, ga1, ga2, ga3)
    gbs = (gb0, gb1, gb2, gb3)

    barrier = pltpu.get_barrier_semaphore()
    for i in range(1, N_COL):
        pl.semaphore_signal(barrier, inc=1, device_id=(rho, lax.rem(col + i, N_COL)), device_id_type=MESH)
    for i in range(1, N_ROW):
        pl.semaphore_signal(barrier, inc=1, device_id=(lax.rem(rho + i, N_ROW), col), device_id_type=MESH)
    diagonals = ((-1, -1), (-1, 1), (1, -1), (1, 1))

    def exists(dr, dc):
        ok = None
        for at, step, size in ((rho, dr, N_ROW), (col, dc, N_COL)):
            if step:
                here = (at > 0) if step < 0 else (at < size - 1)
                ok = here if ok is None else jnp.logical_and(ok, here)
        return ok

    for dr, dc in diagonals:
        @pl.when(exists(dr, dc))
        def _():
            pl.semaphore_signal(barrier, inc=1, device_id=(rho + dr, col + dc), device_id_type=MESH)

    mwin[MARGIN : MARGIN + CR, 0:CC] = cond[...] * mask[...].astype(F32)

    def land(dr, dc):
        rows = {-1: pl.ds(0, MARGIN), 0: pl.ds(MARGIN, CR), 1: pl.ds(MARGIN + CR, MARGIN)}[dr]
        if dc == 0:
            return mwin.at[rows, pl.ds(0, CC)]
        return (side_r if dc > 0 else side_l).at[rows, :]

    def take(dr, dc):
        rows = {-1: pl.ds(MARGIN, MARGIN), 0: pl.ds(MARGIN, CR), 1: pl.ds(MARGIN + CR - MARGIN, MARGIN)}[dr]
        cols = {-1: pl.ds(0, 128), 0: pl.ds(0, CC), 1: pl.ds(CC - 128, 128)}[dc]
        return mwin.at[rows, cols]

    around = [(dr, dc) for dr in (-1, 0, 1) for dc in (-1, 0, 1) if dr or dc]
    for dr, dc in around:
        @pl.when(jnp.logical_not(exists(dr, dc)))
        def _():
            ref = land(dr, dc)
            ref[...] = jnp.zeros(ref.shape, F32)

    def halo_copy(n, dr, dc):
        m = around.index((-dr, -dc))
        return pltpu.make_async_remote_copy(
            src_ref=take(dr, dc), dst_ref=land(-dr, -dc),
            send_sem=halo_send.at[n], recv_sem=halo_recv.at[m],
            device_id=(rho + dr, col + dc), device_id_type=MESH,
        )

    gflat = flat_row(gidx[...].astype(F32)).astype(jnp.int32)
    sflat = flat_row(sidx[...].astype(F32)).astype(jnp.int32)
    cflat = flat_row(scur[...])
    g_row, g_col = gflat // NC, gflat % NC
    s_row, s_col = sflat // NC, sflat % NC

    expected = N_COL - 1 + N_ROW - 1
    for dr, dc in diagonals:
        expected = expected + exists(dr, dc).astype(jnp.int32)
    pl.semaphore_wait(barrier, expected)

    for n, (dr, dc) in enumerate(around):
        @pl.when(exists(dr, dc))
        def _():
            halo_copy(n, dr, dc).start()

    own_b = iota((NB, 256), 1) // 16 == iota((NB, 256), 0)
    g_rel = g_row - rho * CR + MARGIN
    s_rel = s_row - rho * CR + MARGIN
    c_hi = cflat.astype(BF16).astype(F32)
    c_mid = (cflat - c_hi).astype(BF16).astype(F32)
    c_lo = cflat - c_hi - c_mid

    def build(r, carry):
        g_hit = jnp.logical_and(own_b, g_rel == r)
        s_hit = jnp.logical_and(own_b, s_rel == r)
        lhs_g[r] = jnp.where(g_hit, 1.0, 0.0).astype(BF16)
        lhs_s[r, :, 0:256] = jnp.where(s_hit, c_hi, 0.0).astype(BF16)
        lhs_s[r, :, 256:512] = jnp.where(s_hit, c_mid, 0.0).astype(BF16)
        lhs_s[r, :, 512:768] = jnp.where(s_hit, c_lo, 0.0).astype(BF16)
        return carry

    lax.fori_loop(0, WR, build, 0)

    def place(column):
        rel = column - col * CC
        return jnp.where(rel >= 576, -1, jnp.where(rel >= 0, rel, jnp.where(rel >= -64, rel + WC, -1)))

    g_hot = jnp.where(place(g_col) == iota((WC, 256), 0), 1.0, 0.0).astype(BF16)
    s_one = jnp.where(place(s_col) == iota((WC, 256), 0), 1.0, 0.0).astype(BF16)
    s_hot = jnp.concatenate([s_one, s_one, s_one], axis=1)

    STEP = 16

    def spread(i, carry):
        rows = pl.ds(i * STEP, STEP)
        diag[rows] = lax.dot_general(
            lhs_g[rows].reshape(STEP * NB, 256), g_hot, NT, preferred_element_type=F32
        ).reshape(STEP, NB, WC)
        hsrc[rows] = lax.dot_general(
            lhs_s[rows].reshape(STEP * NB, 768), s_hot, NT, preferred_element_type=F32
        ).reshape(STEP, NB, WC)
        return carry

    lax.fori_loop(0, WR // STEP, spread, 0)

    a1 = jnp.where(g_col // CC == iota((8, 256), 0), 1.0, 0.0).astype(BF16)
    a2 = jnp.where(
        jnp.logical_and(
            g_row // CR == iota((256, 256), 0) // 16,
            iota((256, 256), 1) // 16 == iota((256, 256), 0) % 16,
        ), 1.0, 0.0).astype(BF16)
    shunt_total = lax.dot_general(a1, a2, NT, preferred_element_type=F32)

    for n, (dr, dc) in enumerate(around):
        @pl.when(exists(dr, dc))
        def _():
            halo_copy(n, dr, dc).wait_send()
            ref = land(dr, dc)
            pltpu.make_async_remote_copy(
                src_ref=ref, dst_ref=ref, send_sem=halo_send.at[n], recv_sem=halo_recv.at[n],
                device_id=(rho + dr, col + dc), device_id_type=MESH,
            ).wait_recv()
    lane = iota((WR, 128), 1)
    mwin[0:WR, CC:WC] = jnp.where(lane < 64, side_r[...], side_l[...])
    mwin[WR : WR + 8, :] = jnp.zeros((8, WC), F32)

    m = mwin[0:WR, :]
    m_s = mwin[1 : WR + 1, :]
    present = jnp.where(m > 0.0, 1.0, 0.0)
    present_s = jnp.where(m_s > 0.0, 1.0, 0.0)
    east = 0.5 * present * roll(present, -1) * (m + roll(m, -1))
    south = 0.5 * present * present_s * (m + m_s)
    west = roll(east, 1)
    mrow[0] = south
    north = jnp.concatenate([jnp.zeros((1, WC), F32), mrow[0, 0 : WR - 1, :]], axis=0)
    base = east + west + south + north + LEAKAGE
    mrow[1] = base
    mrow[2] = east
    mrow[3] = present
    at_r = iota((WR, WC), 0)
    at_c = iota((WR, WC), 1)
    row_in = jnp.where(jnp.logical_and(at_r >= MARGIN, at_r < MARGIN + CR), 1.0, 0.0)
    row_in_s = jnp.where(jnp.logical_and(at_r >= MARGIN - 1, at_r < MARGIN + CR - 1), 1.0, 0.0)
    row_in_n = jnp.where(jnp.logical_and(at_r >= MARGIN + 1, at_r < MARGIN + CR + 1), 1.0, 0.0)
    col_in = jnp.where(at_c < CC, 1.0, 0.0)
    col_in_e = jnp.where(jnp.logical_or(at_c < CC - 1, at_c == WC - 1), 1.0, 0.0)
    col_in_w = jnp.where(jnp.logical_and(at_c >= 1, at_c <= CC), 1.0, 0.0)
    inside = row_in * col_in
    mrow[4] = (
        base * inside - east * (row_in * col_in_e) - west * (row_in * col_in_w)
        - south * (row_in_s * col_in) - north * (row_in_n * col_in)
    )
    gap_field = ((((base - east) - west) - south) - north - LEAKAGE) * inside
    east_field = jnp.where(at_c == CC - 1, east * row_in, 0.0)
    south_field = jnp.where(at_r == MARGIN + CR - 1, south * col_in, 0.0)

    def total(field):
        return jnp.sum(jnp.sum(field, axis=0, keepdims=True), axis=1, keepdims=True)

    slot = iota((NB, 128), 1) // 16
    own_slot = slot == lax.rem(rho, 8)
    same_b = iota((NB, 128), 1) % 16 == iota((NB, 128), 0)
    row_slot = iota((1, 128), 1) // 16 == lax.rem(rho, 8)

    def one_row(value):
        return jnp.where(row_slot, jnp.broadcast_to(value, (1, 128)), 0.0)

    def b_row(acc, where):
        value = jnp.sum(acc, axis=1, keepdims=True)
        return jnp.sum(jnp.where(jnp.logical_and(where, same_b), value, 0.0), axis=0, keepdims=True)

    def fold(x):
        parts = [x[:, 128 * i : 128 * (i + 1)] for i in range(x.shape[1] // 128)]
        acc = parts[0]
        for p in parts[1:]:
            acc = acc + p
        return acc

    def send_a(g, rows):
        ga = gas[g]
        ga[col] = jnp.concatenate(rows, axis=0)
        for i in range(1, N_COL):
            pltpu.make_async_remote_copy(
                src_ref=ga.at[col], dst_ref=ga.at[col], send_sem=ga_send.at[g], recv_sem=ga_recv.at[g],
                device_id=(rho, lax.rem(col + i, N_COL)), device_id_type=MESH,
            ).start()

    def send_b(g):
        ga, gb = gas[g], gbs[g]
        peers = pl.ds(0, N_COL - 1)
        pltpu.make_async_remote_copy(
            src_ref=ga.at[peers], dst_ref=ga.at[peers], send_sem=ga_send.at[g], recv_sem=ga_recv.at[g],
            device_id=(rho, lax.rem(col + 1, N_COL)), device_id_type=MESH,
        ).wait()
        for i in range(1, N_ROW):
            pltpu.make_async_remote_copy(
                src_ref=ga, dst_ref=gb.at[rho], send_sem=gb_send.at[g], recv_sem=gb_recv.at[g],
                device_id=(lax.rem(rho + i, N_ROW), col), device_id_type=MESH,
            ).start()
        gb[rho] = ga[...]

    def wait_b(g):
        gb = gbs[g]
        peers = pl.ds(0, N_ROW - 1)
        pltpu.make_async_remote_copy(
            src_ref=gb.at[peers], dst_ref=gb.at[peers], send_sem=gb_send.at[g], recv_sem=gb_recv.at[g],
            device_id=(lax.rem(rho + 1, N_ROW), col), device_id_type=MESH,
        ).wait()

    def coarse(g, k):
        gb = gbs[g]
        halves = []
        for h in range(2):
            acc = gb[8 * h, :, k, :]
            for i in range(1, 8):
                acc = acc + gb[8 * h + i, :, k, :]
            halves.append(acc)
        return jnp.concatenate(halves, axis=1)

    def mask_rows(r, carry):
        here = hsrc[r] * mrow[3, pl.ds(r, 1), :]
        hsrc[r] = here
        return carry

    lax.fori_loop(0, WR, mask_rows, 0, unroll=4)

    def sum_rows(r, acc):
        return acc + fold(hsrc[r, :, 0:CC])

    inflow_acc = lax.fori_loop(MARGIN, MARGIN + CR, sum_rows, jnp.zeros((NB, 128), F32), unroll=4)
    send_a(0, [
        b_row(inflow_acc, own_slot), one_row(total(east_field)), one_row(total(south_field)), one_row(total(gap_field)),
    ])

    def coeffs(r, carry):
        rows = pl.ds(r, 1)
        d = diag[r] + mrow[1, rows, :]
        inverse = RELAXATION / d
        winv[r] = inverse
        s_a[r] = inverse * hsrc[r]
        e_east[r] = jnp.broadcast_to(mrow[2, rows, :], (8, WC))
        e_south[r] = jnp.broadcast_to(mrow[0, rows, :], (8, WC))
        kappa[r] = jnp.broadcast_to(mrow[4, rows, :], (8, WC))
        return carry

    lax.fori_loop(0, WR, coeffs, 0, unroll=2)

    def sweep(src, dst, width, extra=None, image=None):
        def cell(r, half, acc):
            sub = pl.ds(8 * half, 8)
            s = src[r, sub, :]
            e = e_east[r]
            t = e * roll(s, -1) + roll(e * s, 1)
            t = t + e_south[r] * src[r + 1, sub, :] + e_south[r - 1] * src[r - 1, sub, :]
            if dst is not None:
                new = s * (1.0 / 3.0) + winv[r, sub, :] * t
                if extra is not None:
                    new = new + extra[r, sub, :]
                dst[r, sub, :] = new
            if acc is not None:
                si = s[:, 0:CC]
                d = diag[r, sub, 0:CC] + mrow[1, pl.ds(r, 1), 0:CC]
                w = d * si - t[:, 0:CC]
                ref, dots = image
                if ref is not None:
                    ref[r - MARGIN, sub, :] = w
                acc = tuple(
                    a + fold((si if f is None else f[r - (0 if f.shape[0] == WR else MARGIN), sub, 0:CC]) * (w if h is None else h[r - MARGIN, sub, :]))
                    for a, (f, h) in zip(acc, dots)
                )
            return acc

        def plain(r, carry):
            cell(r, 0, None)
            cell(r, 1, None)
            return carry

        lo, hi = MARGIN - width, MARGIN + CR + width
        if image is None:
            lax.fori_loop(0, (hi - lo) // 2, lambda i, c: plain(lo + 2 * i + 1, plain(lo + 2 * i, c)), 0)
            return None
        if lo < MARGIN:
            lax.fori_loop(lo, MARGIN, plain, 0)
            lax.fori_loop(MARGIN + CR, hi, plain, 0)
        zero = tuple(jnp.zeros((8, 128), F32) for _ in image[1])

        def rich(r, carry):
            return cell(r, 0, carry[0]), cell(r, 1, carry[1])

        top, bottom = lax.fori_loop(MARGIN, MARGIN + CR, rich, (zero, zero))
        return [jnp.concatenate([a, b], axis=0) for a, b in zip(top, bottom)]

    def block_image(field, also=None):
        def step(r, carry):
            acc, acc2 = carry
            f = field[r]
            k = kappa[r]
            acc = acc + fold(f * jnp.concatenate([k, k], axis=0))
            return acc, acc2

        def inner(r, carry):
            acc, acc2 = step(r, carry)
            fi = field[r, :, 0:CC]
            acc = acc + fold(fi * diag[r, :, 0:CC])
            if also is not None:
                acc2 = acc2 + fold(fi * also[r, :, 0:CC])
            return acc, acc2

        zero = jnp.zeros((NB, 128), F32)
        carry = step(MARGIN - 1, (zero, zero))
        carry = lax.fori_loop(MARGIN, MARGIN + CR, inner, carry, unroll=2)
        return step(MARGIN + CR, carry)

    def keep(r, carry):
        v1[r] = s_a[r]
        return carry

    lax.fori_loop(0, WR, keep, 0, unroll=2)
    sweep(v1, s_a, 14, extra=v1)
    sweep(s_a, s_b, 13, extra=v1)
    send_b(0)
    sweep(s_b, s_a, 12, extra=v1)
    sweep(s_a, s_b, 11, extra=v1)
    ra, ru = block_image(s_b, hsrc)
    zero_row = jnp.zeros((1, 128), F32)
    send_a(1, [b_row(ra, own_slot), zero_row])

    wait_b(0)
    f0 = coarse(0, 0)
    ec = coarse(0, 1)
    sc = coarse(0, 2)
    gap = coarse(0, 3)
    degree = LEAKAGE * CR * CC + shunt_total + ec + pltpu.roll(ec, 1, 0) + sc + roll(sc, 16)
    sub = iota((8, 256), 0)
    t = []
    for j in range(8):
        tj = jnp.where(sub == j, degree, 0.0)
        tj = jnp.where(sub == j - 1, -ec, tj)
        tj = jnp.where(sub == j + 1, -jnp.broadcast_to(ec[j : j + 1, :], (8, 256)), tj)
        t.append(tj)
    uvec = -sc
    lvec = roll(uvec, 16)
    x = mat_inv(t)
    for j in range(8):
        cfac[0, j] = x[j]
    ux = [uvec * x[j] for j in range(8)]
    lx = [lvec * x[j] for j in range(8)]
    p = [ux[j] * uvec[j : j + 1, :] for j in range(8)]
    q = [lx[j] * lvec[j : j + 1, :] for j in range(8)]
    w = [ux[j] * lvec[j : j + 1, :] for j in range(8)]
    wt = [lx[j] * uvec[j : j + 1, :] for j in range(8)]
    for level in range(1, 5):
        d = 16 << (level - 1)
        t = [t[j] - roll(p[j], d) - roll(q[j], -d) for j in range(8)]
        x = mat_inv(t)
        for j in range(8):
            cfac[level, j] = x[j]
        if level == 4:
            break
        low = [-roll(w[j], d) for j in range(8)]
        up = [-roll(wt[j], -d) for j in range(8)]
        low_t = [-roll(wt[j], d) for j in range(8)]
        up_t = [-roll(w[j], -d) for j in range(8)]
        for j in range(8):
            clow[level - 1, j] = low[j]
            cup[level - 1, j] = up[j]
        y = mat_mat(x, up)
        z = mat_mat(x, low)
        p = mat_mat(up_t, y)
        q = mat_mat(low_t, z)
        w = mat_mat(up_t, z)
        wt = mat_mat(low_t, y)

    def solve(f):
        h = mat_vec([cfac[0, j] for j in range(8)], f)
        f = f - lvec * roll(h, 16) - uvec * roll(h, -16)
        for level in range(1, 4):
            d = 16 << level
            h = mat_vec([cfac[level, j] for j in range(8)], f)
            f = f - mat_vec([clow[level - 1, j] for j in range(8)], roll(h, d))
            f = f - mat_vec([cup[level - 1, j] for j in range(8)], roll(h, -d))
        return mat_vec([cfac[4, j] for j in range(8)], f)

    wide_b = iota((NB, 256), 1) % 16 == iota((NB, 256), 0)

    def to_b(row):
        return jnp.sum(jnp.where(wide_b, row, 0.0), axis=1, keepdims=True)

    def dot_c(a, b):
        return to_b(jnp.sum(a * b, axis=0, keepdims=True))

    lane_c = iota((NB, WC), 1)

    def around_field(y):
        fields = []
        lane_row = iota((8, 256), 1) // 16
        for dr in (-1, 0, 1):
            vals = []
            for dc in (0, 1, -1):
                hit = jnp.logical_and(lane_row == rho + dr, sub == col + dc)
                vals.append(to_b(jnp.sum(jnp.where(hit, y, 0.0), axis=0, keepdims=True)))
            fields.append(jnp.where(lane_c < CC, vals[0], jnp.where(lane_c < CC + 64, vals[1], vals[2])))
        return fields

    def combine(dst, src, fields, width, sign):
        spans = ((MARGIN - width, MARGIN), (MARGIN, MARGIN + CR), (MARGIN + CR, MARGIN + CR + width))
        for (lo, hi), field in zip(spans, fields):
            def step(r, carry):
                dst[r] = field + src[r] if sign > 0 else field - src[r]
                return carry
            lax.fori_loop(lo, hi, step, 0)

    y0 = solve(f0)
    send_b(1)
    combine(v0, s_b, around_field(y0), 11, 1)

    (mu0,) = sweep(v0, s_a, 10, image=(w0, ((None, None),)))
    sweep(s_a, s_b, 9)
    sweep(s_b, s_a, 8)
    sweep(s_a, s_b, 7)
    sweep(s_b, s_a, 6)
    ra0, _ = block_image(s_a)
    send_a(2, [b_row(ra0, own_slot), zero_row])
    wait_b(1)
    f1 = f0 + coarse(1, 0) + gap * y0
    g0 = solve(f1)
    combine(v1, s_a, around_field(g0), 6, -1)

    mu2, mu1 = sweep(v1, s_b, 5, image=(w1, ((None, None), (None, w0))))
    sweep(s_b, s_a, 4)
    sweep(s_a, s_b, 3)
    send_b(2)
    sweep(s_b, s_a, 2)
    sweep(s_a, s_b, 1)
    bab, bw1 = sweep(s_b, None, 0, image=(None, ((None, None), (None, w1))))
    ra1, _ = block_image(s_b)
    moments = zero_row
    for n, acc in enumerate((ru, mu0, mu1, mu2, bw1, bab)):
        moments = moments + b_row(acc, slot == n)
    send_a(3, [b_row(ra1, own_slot), moments])
    wait_b(2)
    f2 = f1 - coarse(2, 0) + gap * g0
    g1 = solve(f2)
    energy_y = dot_c(f0, y0)
    g1w1 = dot_c(g1, f2)
    g1gap = dot_c(g1, g1 * gap)
    send_b(3)
    wait_b(3)
    ra1_all = coarse(3, 0)
    g1ra1 = dot_c(g1, ra1_all)
    mom = coarse(3, 1)
    mom = jnp.sum(mom[:, 0:128] + mom[:, 128:256], axis=0, keepdims=True)

    def moment(n):
        return jnp.sum(jnp.where(jnp.logical_and(slot == n, same_b), mom, 0.0), axis=1, keepdims=True)

    energy = moment(0) + energy_y
    m0, m1, m2 = moment(1), moment(2), moment(3)
    m3 = g1w1 - moment(4)
    m4 = g1w1 + g1gap - 2.0 * g1ra1 + moment(5)
    r1 = m0 - energy
    r2 = m1 - r1

    def ratio(a, b, scale):
        ok = b > scale
        return jnp.where(ok, a / jnp.where(ok, b, 1.0), 0.0)

    l10 = m1 / m0
    l20 = m2 / m0
    d1 = m2 - l10 * m1
    e21 = m3 - l20 * m1
    l21 = ratio(e21, d1, 0.0)
    d2 = m4 - l20 * m2 - l21 * e21
    t1 = r1 - l10 * energy
    t2 = r2 - l20 * energy - l21 * t1
    c2 = ratio(t2, d2, 0.0)
    c1 = ratio(t1, d1, 0.0) - l21 * c2
    c0 = energy / m0 - l10 * c1 - l20 * c2
    hit = jnp.logical_and(iota((8, 256), 1) // 16 == rho, sub == col)
    shift = c2 * to_b(jnp.sum(jnp.where(hit, g1, 0.0), axis=0, keepdims=True))
    c0 = jnp.broadcast_to(c0, (NB, CC))
    c1 = jnp.broadcast_to(c1, (NB, CC))
    c2 = jnp.broadcast_to(c2, (NB, CC))
    shift = jnp.broadcast_to(shift, (NB, CC))

    def finish(r, carry):
        w = r + MARGIN
        out[r] = c0 * v0[w, :, 0:CC] + c1 * v1[w, :, 0:CC] - c2 * s_b[w, :, 0:CC] + shift
        return carry

    lax.fori_loop(0, CR, finish, 0, unroll=2)


def shards(conductance, nodata_mask, source_index, source_current, ground_index):
    big = pltpu.VMEM((WR, NB, WC), F32)
    edge = pltpu.VMEM((WR, 8, WC), F32)
    own = pltpu.VMEM((CR, NB, CC), F32)
    scratch = [
        pltpu.VMEM((WR + 8, WC), F32), pltpu.VMEM((WR, 128), F32), pltpu.VMEM((WR, 128), F32),
        big, big, big, edge, edge, edge,
        big, big, big, big, own, own,
        pltpu.VMEM((WR, NB, 256), BF16), pltpu.VMEM((WR, NB, 768), BF16),
        pltpu.VMEM((5, 8, 8, 256), F32), pltpu.VMEM((3, 8, 8, 256), F32), pltpu.VMEM((3, 8, 8, 256), F32),
        pltpu.VMEM((5, WR, WC), F32),
    ]
    for q in (4, 2, 2, 2):
        scratch += [pltpu.VMEM((N_COL, q, 128), F32), pltpu.VMEM((N_ROW, N_COL, q, 128), F32)]
    scratch += [pltpu.SemaphoreType.DMA((8,)), pltpu.SemaphoreType.DMA((8,))]
    scratch += [pltpu.SemaphoreType.DMA((4,)) for _ in range(4)]
    voltage = pl.pallas_call(
        body,
        out_shape=jax.ShapeDtypeStruct((CR, NB, CC), F32),
        in_specs=[pl.BlockSpec(memory_space=pltpu.VMEM)] * 5,
        out_specs=pl.BlockSpec(memory_space=pltpu.VMEM),
        scratch_shapes=scratch,
        compiler_params=pltpu.CompilerParams(
            collective_id=0, has_side_effects=True, vmem_limit_bytes=56 * 1024 * 1024
        ),
    )(conductance, nodata_mask, source_index, source_current, ground_index)
    return jnp.transpose(voltage, (1, 0, 2))


def solution(mesh):
    return jax.shard_map(
        shards,
        mesh=mesh,
        in_specs=(P("row", "col"), P("row", "col"), P(), P(), P()),
        out_specs=P(None, "row", "col"),
        check_vma=False,
    )
```

```python
import jax
import jax.numpy as jnp
from jax import lax
from jax.experimental import pallas as pl
from jax.experimental.pallas import tpu as pltpu
from jax.sharding import PartitionSpec as P

LEAKAGE = 0.0001
RELAXATION = 2.0 / 3.0
NB = 16
CR = 32
CC = 512
N_ROW = 16
N_COL = 8
NC = N_COL * CC
MARGIN = 16
STEP_ROWS = 6
WR = CR + 2 * MARGIN
WC = CC + 128
F32 = jnp.float32
BF16 = jnp.bfloat16
MESH = pl.DeviceIdType.MESH
NT = (((1,), (1,)), ((), ()))


def iota(shape, dim):
    return lax.broadcasted_iota(jnp.int32, shape, dim)


def roll(x, shift):
    return pltpu.roll(x, shift % x.shape[-1], x.ndim - 1)


def at_col():
    c = iota((1, WC), 1)
    return 5 * (c % 128) + c // 128


def tiles(x):
    return [x[..., 128 * j : 128 * (j + 1)] for j in range(WC // 128)]


def east_of(x):
    t = tiles(x)
    return jnp.concatenate(t[1:] + [roll(t[0], -1)], axis=-1)


def west_of(x):
    t = tiles(x)
    return jnp.concatenate([roll(t[-1], 1)] + t[:-1], axis=-1)


def interleave(x):
    n = x.shape[0]
    lane = iota((n, 128), 1)
    source = tiles(x)
    out = []
    for j in range(5):
        p = 5 * lane + j
        part = None
        for t in range(5):
            got = jnp.take_along_axis(source[t], p % 128, axis=1)
            part = got if part is None else jnp.where(p // 128 == t, got, part)
        out.append(part)
    return jnp.concatenate(out, axis=1)


def natural(parts):
    n = parts[0].shape[0]
    lane = iota((n, 128), 1)
    out = []
    for t in range(CC // 128):
        c = 128 * t + lane
        fifth = (c * 52429) >> 18
        j_of = c - 5 * fifth
        tile = None
        for j in range(5):
            got = jnp.take_along_axis(parts[j], fifth, axis=1)
            tile = got if tile is None else jnp.where(j_of == j, got, tile)
        out.append(tile)
    return jnp.concatenate(out, axis=1)


def flat_row(x):
    pick = (iota((16, 256), 1) % 16 == iota((16, 256), 0)).astype(F32)
    tiled = jnp.dot(x, pick, precision=lax.Precision.HIGHEST, preferred_element_type=F32)
    own = iota((16, 256), 1) // 16 == iota((16, 256), 0)
    return jnp.sum(jnp.where(own, tiled, 0.0), axis=0, keepdims=True)


def mat_mat(a, b):
    out = []
    for j in range(8):
        total = a[0] * b[j][0:1, :]
        for k in range(1, 8):
            total = total + a[k] * b[j][k : k + 1, :]
        out.append(total)
    return out


def mat_vec(a, f):
    parts = [a[k] * f[k : k + 1, :] for k in range(8)]
    while len(parts) > 1:
        parts = [parts[i] + parts[i + 1] for i in range(0, len(parts), 2)]
    return parts[0]


def mat_inv(t):
    t = list(t)
    sub = iota((8, 256), 0)
    for k in range(8):
        pivot = 1.0 / t[k][k : k + 1, :]
        column = t[k]
        at_k = sub == k
        for j in range(8):
            if j != k:
                row = t[j][k : k + 1, :] * pivot
                t[j] = jnp.where(at_k, row, t[j] - column * row)
        t[k] = jnp.where(at_k, pivot, -column * pivot)
    return t


def body(
    cond, mask, sidx, scur, gidx, out,
    mwin, side_r, side_l, diag, hsrc, winv3, e_east, e_south, kappa,
    s_a, s_b, v0, v1, w0, w1, lhs_g, lhs_s, cfac, clow, cup, mrow,
    ga0, gb0, ga1, gb1, ga2, gb2, ga3, gb3,
    nat, coef, halo_send, halo_recv, ga_send, ga_recv, gb_send, gb_recv,
):
    rho = lax.axis_index("row")
    col = lax.axis_index("col")
    gas = (ga0, ga1, ga2, ga3)
    gbs = (gb0, gb1, gb2, gb3)

    barrier = pltpu.get_barrier_semaphore()
    for i in range(1, N_COL):
        pl.semaphore_signal(barrier, inc=1, device_id=(rho, lax.rem(col + i, N_COL)), device_id_type=MESH)
    for i in range(1, N_ROW):
        pl.semaphore_signal(barrier, inc=1, device_id=(lax.rem(rho + i, N_ROW), col), device_id_type=MESH)
    diagonals = ((-1, -1), (-1, 1), (1, -1), (1, 1))

    def exists(dr, dc):
        ok = None
        for at, step, size in ((rho, dr, N_ROW), (col, dc, N_COL)):
            if step:
                here = (at > 0) if step < 0 else (at < size - 1)
                ok = here if ok is None else jnp.logical_and(ok, here)
        return ok

    for dr, dc in diagonals:
        @pl.when(exists(dr, dc))
        def _():
            pl.semaphore_signal(barrier, inc=1, device_id=(rho + dr, col + dc), device_id_type=MESH)

    mwin[MARGIN : MARGIN + CR, 0:CC] = cond[...] * mask[...].astype(F32)

    def land(dr, dc):
        rows = {-1: pl.ds(0, MARGIN), 0: pl.ds(MARGIN, CR), 1: pl.ds(MARGIN + CR, MARGIN)}[dr]
        if dc == 0:
            return mwin.at[rows, pl.ds(0, CC)]
        return (side_r if dc > 0 else side_l).at[rows, :]

    def take(dr, dc):
        rows = {-1: pl.ds(MARGIN, MARGIN), 0: pl.ds(MARGIN, CR), 1: pl.ds(MARGIN + CR - MARGIN, MARGIN)}[dr]
        cols = {-1: pl.ds(0, 128), 0: pl.ds(0, CC), 1: pl.ds(CC - 128, 128)}[dc]
        return mwin.at[rows, cols]

    around = [(dr, dc) for dr in (-1, 0, 1) for dc in (-1, 0, 1) if dr or dc]
    for dr, dc in around:
        @pl.when(jnp.logical_not(exists(dr, dc)))
        def _():
            ref = land(dr, dc)
            ref[...] = jnp.zeros(ref.shape, F32)

    def halo_copy(n, dr, dc):
        m = around.index((-dr, -dc))
        return pltpu.make_async_remote_copy(
            src_ref=take(dr, dc), dst_ref=land(-dr, -dc),
            send_sem=halo_send.at[n], recv_sem=halo_recv.at[m],
            device_id=(rho + dr, col + dc), device_id_type=MESH,
        )

    gflat = flat_row(gidx[...].astype(F32)).astype(jnp.int32)
    sflat = flat_row(sidx[...].astype(F32)).astype(jnp.int32)
    cflat = flat_row(scur[...])
    g_row, g_col = gflat // NC, gflat % NC
    s_row, s_col = sflat // NC, sflat % NC

    expected = N_COL - 1 + N_ROW - 1
    for dr, dc in diagonals:
        expected = expected + exists(dr, dc).astype(jnp.int32)
    pl.semaphore_wait(barrier, expected)

    for n, (dr, dc) in enumerate(around):
        @pl.when(exists(dr, dc))
        def _():
            halo_copy(n, dr, dc).start()

    own_b = iota((NB, 256), 1) // 16 == iota((NB, 256), 0)
    g_rel = g_row - rho * CR + MARGIN
    s_rel = s_row - rho * CR + MARGIN
    c_hi = cflat.astype(BF16).astype(F32)
    c_mid = (cflat - c_hi).astype(BF16).astype(F32)
    c_lo = cflat - c_hi - c_mid

    def build(r, carry):
        g_hit = jnp.logical_and(own_b, g_rel == r)
        s_hit = jnp.logical_and(own_b, s_rel == r)
        lhs_g[r] = jnp.where(g_hit, 1.0, 0.0).astype(BF16)
        lhs_s[r, :, 0:256] = jnp.where(s_hit, c_hi, 0.0).astype(BF16)
        lhs_s[r, :, 256:512] = jnp.where(s_hit, c_mid, 0.0).astype(BF16)
        lhs_s[r, :, 512:768] = jnp.where(s_hit, c_lo, 0.0).astype(BF16)
        return carry

    lax.fori_loop(0, WR, build, 0)

    def place(column):
        rel = column - col * CC
        return jnp.where(rel >= 576, -1, jnp.where(rel >= 0, rel, jnp.where(rel >= -64, rel + WC, -1)))

    spot = 5 * (iota((WC, 256), 0) % 128) + iota((WC, 256), 0) // 128
    g_hot = jnp.where(place(g_col) == spot, 1.0, 0.0).astype(BF16)
    s_one = jnp.where(place(s_col) == spot, 1.0, 0.0).astype(BF16)
    s_hot = jnp.concatenate([s_one, s_one, s_one], axis=1)

    STEP = 16

    def spread(i, carry):
        rows = pl.ds(i * STEP, STEP)
        diag[rows] = lax.dot_general(
            lhs_g[rows].reshape(STEP * NB, 256), g_hot, NT, preferred_element_type=F32
        ).reshape(STEP, NB, WC)
        hsrc[rows] = lax.dot_general(
            lhs_s[rows].reshape(STEP * NB, 768), s_hot, NT, preferred_element_type=F32
        ).reshape(STEP, NB, WC)
        return carry

    lax.fori_loop(0, WR // STEP, spread, 0)

    a1 = jnp.where(g_col // CC == iota((8, 256), 0), 1.0, 0.0).astype(BF16)
    a2 = jnp.where(
        jnp.logical_and(
            g_row // CR == iota((256, 256), 0) // 16,
            iota((256, 256), 1) // 16 == iota((256, 256), 0) % 16,
        ), 1.0, 0.0).astype(BF16)
    shunt_total = lax.dot_general(a1, a2, NT, preferred_element_type=F32)

    for n, (dr, dc) in enumerate(around):
        @pl.when(exists(dr, dc))
        def _():
            halo_copy(n, dr, dc).wait_send()
            ref = land(dr, dc)
            pltpu.make_async_remote_copy(
                src_ref=ref, dst_ref=ref, send_sem=halo_send.at[n], recv_sem=halo_recv.at[n],
                device_id=(rho + dr, col + dc), device_id_type=MESH,
            ).wait_recv()
    lane = iota((WR, 128), 1)
    mwin[0:WR, CC:WC] = jnp.where(lane < 64, side_r[...], side_l[...])

    m = interleave(mwin[...])
    mrow[0] = m
    last = jnp.zeros((1, WC), F32)
    m_s = jnp.concatenate([mrow[0, 1:WR, :], last], axis=0)
    present = jnp.where(m > 0.0, 1.0, 0.0)
    present_s = jnp.where(m_s > 0.0, 1.0, 0.0)
    east = 0.5 * present * east_of(present) * (m + east_of(m))
    south = 0.5 * present * present_s * (m + m_s)
    west = west_of(east)
    mrow[0] = south
    north = jnp.concatenate([last, mrow[0, 0 : WR - 1, :]], axis=0)
    base = east + west + south + north + LEAKAGE
    mrow[1] = base
    mrow[2] = east
    mrow[3] = present
    at_r = iota((WR, WC), 0)
    at_c = jnp.broadcast_to(at_col(), (WR, WC))
    row_in = jnp.where(jnp.logical_and(at_r >= MARGIN, at_r < MARGIN + CR), 1.0, 0.0)
    row_in_s = jnp.where(jnp.logical_and(at_r >= MARGIN - 1, at_r < MARGIN + CR - 1), 1.0, 0.0)
    row_in_n = jnp.where(jnp.logical_and(at_r >= MARGIN + 1, at_r < MARGIN + CR + 1), 1.0, 0.0)
    col_in = jnp.where(at_c < CC, 1.0, 0.0)
    col_in_e = jnp.where(jnp.logical_or(at_c < CC - 1, at_c == WC - 1), 1.0, 0.0)
    col_in_w = jnp.where(jnp.logical_and(at_c >= 1, at_c <= CC), 1.0, 0.0)
    inside = row_in * col_in
    mrow[4] = (
        base * inside - east * (row_in * col_in_e) - west * (row_in * col_in_w)
        - south * (row_in_s * col_in) - north * (row_in_n * col_in)
    )
    mrow[5] = inside
    gap_field = ((((base - east) - west) - south) - north - LEAKAGE) * inside
    east_field = jnp.where(at_c == CC - 1, east * row_in, 0.0)
    south_field = jnp.where(at_r == MARGIN + CR - 1, south * col_in, 0.0)

    def total(field):
        return jnp.sum(jnp.sum(field, axis=0, keepdims=True), axis=1, keepdims=True)

    slot = iota((NB, 128), 1) // 16
    own_slot = slot == lax.rem(rho, 8)
    same_b = iota((NB, 128), 1) % 16 == iota((NB, 128), 0)
    row_slot = iota((1, 128), 1) // 16 == lax.rem(rho, 8)

    def one_row(value):
        return jnp.where(row_slot, jnp.broadcast_to(value, (1, 128)), 0.0)

    def b_row(acc, where):
        value = jnp.sum(acc, axis=1, keepdims=True)
        return jnp.sum(jnp.where(jnp.logical_and(where, same_b), value, 0.0), axis=0, keepdims=True)

    own_col = at_col() < CC

    def fold(x):
        parts = tiles(jnp.where(own_col, x, 0.0))
        return parts[0] + parts[1] + ((parts[2] + parts[3]) + parts[4])

    def put_natural(n, field, lo, hi):
        def step(r, carry):
            for half in range(2):
                sub = pl.ds(8 * half, 8)
                nat[n, sub, r, :] = natural(tiles(field[r + MARGIN, sub, :]))
            return carry

        lax.fori_loop(lo, hi, step, 0, unroll=4)

    def send_a(g, rows):
        ga = gas[g]
        ga[rho] = jnp.concatenate(rows, axis=0)
        for i in range(1, N_ROW):
            pltpu.make_async_remote_copy(
                src_ref=ga.at[rho], dst_ref=ga.at[rho], send_sem=ga_send.at[g], recv_sem=ga_recv.at[g],
                device_id=(lax.rem(rho + i, N_ROW), col), device_id_type=MESH,
            ).start()

    def send_b(g):
        ga, gb = gas[g], gbs[g]
        peers = pl.ds(0, N_ROW - 1)
        pltpu.make_async_remote_copy(
            src_ref=ga.at[peers], dst_ref=ga.at[peers], send_sem=ga_send.at[g], recv_sem=ga_recv.at[g],
            device_id=(lax.rem(rho + 1, N_ROW), col), device_id_type=MESH,
        ).wait()
        for h in range(2):
            acc = ga[8 * h]
            for i in range(1, 8):
                acc = acc + ga[8 * h + i]
            gb[col, h] = acc
        for i in range(1, N_COL):
            pltpu.make_async_remote_copy(
                src_ref=gb.at[col], dst_ref=gb.at[col], send_sem=gb_send.at[g], recv_sem=gb_recv.at[g],
                device_id=(rho, lax.rem(col + i, N_COL)), device_id_type=MESH,
            ).start()

    def wait_b(g):
        gb = gbs[g]
        peers = pl.ds(0, N_COL - 1)
        pltpu.make_async_remote_copy(
            src_ref=gb.at[peers], dst_ref=gb.at[peers], send_sem=gb_send.at[g], recv_sem=gb_recv.at[g],
            device_id=(rho, lax.rem(col + 1, N_COL)), device_id_type=MESH,
        ).wait()

    def coarse(g, k):
        gb = gbs[g]
        return jnp.concatenate([gb[:, 0, k, :], gb[:, 1, k, :]], axis=1)

    def mask_rows(r, carry):
        here = hsrc[r] * mrow[3, pl.ds(r, 1), :]
        hsrc[r] = here
        return carry + here * mrow[5, pl.ds(r, 1), :]

    wide_zero = jnp.zeros((NB, WC), F32)
    inflow_acc = lax.fori_loop(0, WR, mask_rows, wide_zero, unroll=4)
    send_a(0, [
        b_row(fold(inflow_acc), own_slot), one_row(total(east_field)), one_row(total(south_field)), one_row(total(gap_field)),
    ])

    def coeffs(r, carry):
        rows = pl.ds(r, 1)
        shunt = diag[r]
        d = shunt + mrow[1, rows, :]
        inverse = 2.0 / d
        diag[r] = d
        winv3[r] = inverse
        kappa[r] = mrow[4, rows, :] + shunt * mrow[5, rows, :]
        v1[r] = (1.0 / 3.0) * inverse * hsrc[r]
        e_east[r] = jnp.broadcast_to(mrow[2, rows, :], (8, WC))
        e_south[r] = jnp.broadcast_to(mrow[0, rows, :], (8, WC))
        return carry

    lax.fori_loop(0, WR, coeffs, 0, unroll=2)

    def sweep(src, dst, width, extra=None, scale=None, image=None):
        count = -(-(CR + 2 * width) // STEP_ROWS)
        lo = MARGIN - width - (count * STEP_ROWS - CR - 2 * width) // 2

        def step(i, carry):
            r0 = lo + i * STEP_ROWS
            for k in range(STEP_ROWS):
                r = r0 + k
                e = tiles(e_east[r])
                south_here = tiles(e_south[r])
                south_north = tiles(e_south[r - 1])
                for half in range(2):
                    sub = pl.ds(8 * half, 8)
                    s = tiles(src[r, sub, :])
                    below = tiles(src[r + 1, sub, :])
                    above = tiles(src[r - 1, sub, :])
                    w3 = tiles(winv3[r, sub, :])
                    h = None if extra is None else tiles(extra[r, sub, :])
                    to_east = s[1:] + [roll(s[0], -1)]
                    flow = [e[j] * s[j] for j in range(4)]
                    to_west = [roll(e[4] * s[4], 1)] + flow
                    for j in range(5):
                        t = (e[j] * to_east[j] + to_west[j]) + (south_here[j] * below[j] + south_north[j] * above[j])
                        at = pl.ds(128 * j, 128)
                        if image is not None:
                            image[r, sub, at] = diag[r, sub, at] * s[j] - t
                        if dst is not None:
                            new = s[j] + w3[j] * t
                            if h is not None:
                                new = new + scale * h[j]
                            dst[r, sub, at] = new
            return carry

        lax.fori_loop(0, count, step, 0)

    def block_image(field):
        acc = lax.fori_loop(
            MARGIN - 1, MARGIN + CR + 1, lambda r, acc: acc + field[r] * kappa[r], wide_zero, unroll=2
        )
        parts = tiles(acc)
        return (parts[0] + parts[1]) + (parts[2] + parts[3]) + parts[4]

    def own_dots(*pairs):
        def step(r, accs):
            return tuple(acc + f[r] * g[r] for acc, (f, g) in zip(accs, pairs))

        accs = lax.fori_loop(MARGIN, MARGIN + CR, step, (wide_zero,) * len(pairs), unroll=2)
        return [fold(acc) for acc in accs]

    sweep(v1, s_a, 14, v1, 3.0)
    sweep(s_a, s_b, 13, v1, 9.0)
    send_b(0)
    sweep(s_b, s_a, 12, v1, 27.0)
    sweep(s_a, s_b, 11, v1, 81.0)
    ra = block_image(s_b) * (1.0 / 81.0)
    zero_row = jnp.zeros((1, 128), F32)
    send_a(1, [b_row(ra, own_slot), zero_row])
    ru = own_dots((s_b, hsrc))[0] * (1.0 / 81.0)

    wait_b(0)
    f0 = coarse(0, 0)
    ec = coarse(0, 1)
    sc = coarse(0, 2)
    gap = coarse(0, 3)
    degree = LEAKAGE * CR * CC + shunt_total + ec + pltpu.roll(ec, 1, 0) + sc + roll(sc, 16)
    sub = iota((8, 256), 0)
    t = []
    for j in range(8):
        tj = jnp.where(sub == j, degree, 0.0)
        tj = jnp.where(sub == j - 1, -ec, tj)
        tj = jnp.where(sub == j + 1, -jnp.broadcast_to(ec[j : j + 1, :], (8, 256)), tj)
        t.append(tj)
    uvec = -sc
    lvec = roll(uvec, 16)
    x = mat_inv(t)
    for j in range(8):
        cfac[0, j] = x[j]
    ux = [uvec * x[j] for j in range(8)]
    lx = [lvec * x[j] for j in range(8)]
    p = [ux[j] * uvec[j : j + 1, :] for j in range(8)]
    q = [lx[j] * lvec[j : j + 1, :] for j in range(8)]
    w = [ux[j] * lvec[j : j + 1, :] for j in range(8)]
    wt = [lx[j] * uvec[j : j + 1, :] for j in range(8)]
    for level in range(1, 5):
        d = 16 << (level - 1)
        t = [t[j] - roll(p[j], d) - roll(q[j], -d) for j in range(8)]
        x = mat_inv(t)
        for j in range(8):
            cfac[level, j] = x[j]
        if level == 4:
            break
        low = [-roll(w[j], d) for j in range(8)]
        up = [-roll(wt[j], -d) for j in range(8)]
        low_t = [-roll(wt[j], d) for j in range(8)]
        up_t = [-roll(w[j], -d) for j in range(8)]
        for j in range(8):
            clow[level - 1, j] = low[j]
            cup[level - 1, j] = up[j]
        y = mat_mat(x, up)
        z = mat_mat(x, low)
        p = mat_mat(up_t, y)
        q = mat_mat(low_t, z)
        w = mat_mat(up_t, z)
        wt = mat_mat(low_t, y)

    def solve(f):
        h = mat_vec([cfac[0, j] for j in range(8)], f)
        f = f - lvec * roll(h, 16) - uvec * roll(h, -16)
        for level in range(1, 4):
            d = 16 << level
            h = mat_vec([cfac[level, j] for j in range(8)], f)
            f = f - mat_vec([clow[level - 1, j] for j in range(8)], roll(h, d))
            f = f - mat_vec([cup[level - 1, j] for j in range(8)], roll(h, -d))
        return mat_vec([cfac[4, j] for j in range(8)], f)

    wide_b = iota((NB, 256), 1) % 16 == iota((NB, 256), 0)

    def to_b(row):
        return jnp.sum(jnp.where(wide_b, row, 0.0), axis=1, keepdims=True)

    def dot_c(a, b):
        return to_b(jnp.sum(a * b, axis=0, keepdims=True))

    lane_c = jnp.broadcast_to(at_col(), (NB, WC))

    def around_field(y):
        fields = []
        lane_row = iota((8, 256), 1) // 16
        for dr in (-1, 0, 1):
            vals = []
            for dc in (0, 1, -1):
                hit = jnp.logical_and(lane_row == rho + dr, sub == col + dc)
                vals.append(to_b(jnp.sum(jnp.where(hit, y, 0.0), axis=0, keepdims=True)))
            fields.append(jnp.where(lane_c < CC, vals[0], jnp.where(lane_c < CC + 64, vals[1], vals[2])))
        return fields

    def combine(dst, src, fields, width, scale):
        spans = ((MARGIN - width, MARGIN), (MARGIN, MARGIN + CR), (MARGIN + CR, MARGIN + CR + width))
        for (lo, hi), field in zip(spans, fields):
            def step(r, carry):
                dst[r] = field + scale * src[r]
                return carry
            lax.fori_loop(lo, hi, step, 0, unroll=2 if (hi - lo) % 2 == 0 else 1)

    y0 = solve(f0)
    combine(v0, s_b, around_field(y0), 11, 1.0 / 81.0)

    sweep(v0, s_a, 10, image=w0)
    send_b(1)
    sweep(s_a, s_b, 9)
    sweep(s_b, s_a, 8)
    sweep(s_a, s_b, 7)
    sweep(s_b, s_a, 6)
    ra0 = block_image(s_a) * (1.0 / 243.0)
    send_a(2, [b_row(ra0, own_slot), zero_row])
    wait_b(1)
    f1 = f0 + coarse(1, 0) + gap * y0
    g0 = solve(f1)
    combine(v1, s_a, around_field(g0), 6, -1.0 / 243.0)

    sweep(v1, s_b, 5, image=w1)
    sweep(s_b, s_a, 4)
    sweep(s_a, s_b, 3)
    sweep(s_b, s_a, 2)
    sweep(s_a, s_b, 1)
    mu0, mu1, mu2 = own_dots((v0, w0), (v1, w0), (v1, w1))
    sweep(s_b, None, 0, image=s_a)
    send_b(2)
    bab, bw1 = own_dots((s_b, s_a), (s_b, w1))
    bab = bab * (1.0 / (243.0 * 243.0))
    bw1 = bw1 * (1.0 / 243.0)
    ra1 = block_image(s_b) * (1.0 / 243.0)
    moments = zero_row
    for n, acc in enumerate((ru, mu0, mu1, mu2, bw1, bab)):
        moments = moments + b_row(acc, slot == n)
    send_a(3, [b_row(ra1, own_slot), moments])
    for n, field in enumerate((v0, v1, s_b)):
        if n == 1:
            wait_b(2)
            f2 = f1 - coarse(2, 0) + gap * g0
            g1 = solve(f2)
        put_natural(n, field, 0, CR // 2)
        if n == 1:
            send_b(3)
        put_natural(n, field, CR // 2, CR)
    energy_y = dot_c(f0, y0)
    g1w1 = dot_c(g1, f2)
    g1gap = dot_c(g1, g1 * gap)
    wait_b(3)
    ra1_all = coarse(3, 0)
    g1ra1 = dot_c(g1, ra1_all)
    mom = coarse(3, 1)
    mom = jnp.sum(mom[:, 0:128] + mom[:, 128:256], axis=0, keepdims=True)

    def moment(n):
        return jnp.sum(jnp.where(jnp.logical_and(slot == n, same_b), mom, 0.0), axis=1, keepdims=True)

    energy = moment(0) + energy_y
    m0, m1, m2 = moment(1), moment(2), moment(3)
    m3 = g1w1 - moment(4)
    m4 = g1w1 + g1gap - 2.0 * g1ra1 + moment(5)
    r1 = m0 - energy
    r2 = m1 - r1

    def ratio(a, b, scale):
        ok = b > scale
        return jnp.where(ok, a / jnp.where(ok, b, 1.0), 0.0)

    l10 = m1 / m0
    l20 = m2 / m0
    d1 = m2 - l10 * m1
    e21 = m3 - l20 * m1
    l21 = ratio(e21, d1, 0.0)
    d2 = m4 - l20 * m2 - l21 * e21
    t1 = r1 - l10 * energy
    t2 = r2 - l20 * energy - l21 * t1
    c2 = ratio(t2, d2, 0.0)
    c1 = ratio(t1, d1, 0.0) - l21 * c2
    c0 = energy / m0 - l10 * c1 - l20 * c2
    hit = jnp.logical_and(iota((8, 256), 1) // 16 == rho, sub == col)
    shift = c2 * to_b(jnp.sum(jnp.where(hit, g1, 0.0), axis=0, keepdims=True))
    for n, c in enumerate((c0, c1, c2 * (-1.0 / 243.0), shift)):
        coef[n] = jnp.broadcast_to(c, (NB, CC))

    def finish(b, carry):
        w = [coef[n, pl.ds(b, 1), :] for n in range(4)]
        out[b] = w[0] * nat[0, b] + w[1] * nat[1, b] + (w[2] * nat[2, b] + w[3])
        return carry

    lax.fori_loop(0, NB, finish, 0)


def shards(conductance, nodata_mask, source_index, source_current, ground_index):
    big = pltpu.VMEM((WR, NB, WC), F32)
    edge = pltpu.VMEM((WR, 8, WC), F32)
    scratch = [
        pltpu.VMEM((WR, WC), F32), pltpu.VMEM((WR, 128), F32), pltpu.VMEM((WR, 128), F32),
        big, big, big, edge, edge, big,
        big, big, big, big, big, big,
        pltpu.VMEM((WR, NB, 256), BF16), pltpu.VMEM((WR, NB, 768), BF16),
        pltpu.VMEM((5, 8, 8, 256), F32), pltpu.VMEM((3, 8, 8, 256), F32), pltpu.VMEM((3, 8, 8, 256), F32),
        pltpu.VMEM((6, WR, WC), F32),
    ]
    for q in (4, 2, 2, 2):
        scratch += [pltpu.VMEM((N_ROW, q, 128), F32), pltpu.VMEM((N_COL, 2, q, 128), F32)]
    scratch += [pltpu.VMEM((3, NB, CR, CC), F32), pltpu.VMEM((4, NB, CC), F32)]
    scratch += [pltpu.SemaphoreType.DMA((8,)), pltpu.SemaphoreType.DMA((8,))]
    scratch += [pltpu.SemaphoreType.DMA((4,)) for _ in range(4)]
    return pl.pallas_call(
        body,
        out_shape=pltpu.VMEM((NB, CR, CC), F32),
        in_specs=[pl.BlockSpec(memory_space=pltpu.VMEM)] * 5,
        out_specs=pl.BlockSpec(memory_space=pltpu.VMEM),
        scratch_shapes=scratch,
        compiler_params=pltpu.CompilerParams(
            collective_id=0, has_side_effects=True, vmem_limit_bytes=56 * 1024 * 1024
        ),
    )(conductance, nodata_mask, source_index, source_current, ground_index)


def solution(mesh):
    return jax.shard_map(
        shards,
        mesh=mesh,
        in_specs=(P("row", "col"), P("row", "col"), P(), P(), P()),
        out_specs=P(None, "row", "col"),
        check_vma=False,
    )
```

```python
import jax
import jax.numpy as jnp
from jax import lax
from jax.experimental import pallas as pl
from jax.experimental.pallas import tpu as pltpu
from jax.sharding import PartitionSpec as P

LEAKAGE = 0.0001
RELAXATION = 2.0 / 3.0
NB = 16
CR = 32
CC = 512
N_ROW = 16
N_COL = 8
NC = N_COL * CC
MARGIN = 16
EARLY = 24
CHOICES = (6, 12)
WR = CR + 2 * MARGIN
WC = CC + 128
F32 = jnp.float32
BF16 = jnp.bfloat16
MESH = pl.DeviceIdType.MESH
NT = (((1,), (1,)), ((), ()))


def iota(shape, dim):
    return lax.broadcasted_iota(jnp.int32, shape, dim)


def roll(x, shift):
    return pltpu.roll(x, shift % x.shape[-1], x.ndim - 1)


def at_col():
    c = iota((1, WC), 1)
    return 5 * (c % 128) + c // 128


def tiles(x):
    return [x[..., 128 * j : 128 * (j + 1)] for j in range(WC // 128)]


def east_of(x):
    t = tiles(x)
    return jnp.concatenate(t[1:] + [roll(t[0], -1)], axis=-1)


def west_of(x):
    t = tiles(x)
    return jnp.concatenate([roll(t[-1], 1)] + t[:-1], axis=-1)


def interleave(x):
    n = x.shape[0]
    lane = iota((n, 128), 1)
    source = tiles(x)
    out = []
    for j in range(5):
        p = 5 * lane + j
        part = None
        for t in range(5):
            got = jnp.take_along_axis(source[t], p % 128, axis=1)
            part = got if part is None else jnp.where(p // 128 == t, got, part)
        out.append(part)
    return jnp.concatenate(out, axis=1)


def natural(parts):
    n = parts[0].shape[0]
    lane = iota((n, 128), 1)
    out = []
    for t in range(CC // 128):
        c = 128 * t + lane
        fifth = (c * 52429) >> 18
        j_of = c - 5 * fifth
        tile = None
        for j in range(5):
            got = jnp.take_along_axis(parts[j], fifth, axis=1)
            tile = got if tile is None else jnp.where(j_of == j, got, tile)
        out.append(tile)
    return jnp.concatenate(out, axis=1)


def flat_row(x):
    pick = (iota((16, 256), 1) % 16 == iota((16, 256), 0)).astype(F32)
    tiled = jnp.dot(x, pick, precision=lax.Precision.HIGHEST, preferred_element_type=F32)
    own = iota((16, 256), 1) // 16 == iota((16, 256), 0)
    return jnp.sum(jnp.where(own, tiled, 0.0), axis=0, keepdims=True)


def mat_mat(a, b):
    out = []
    for j in range(8):
        total = a[0] * b[j][0:1, :]
        for k in range(1, 8):
            total = total + a[k] * b[j][k : k + 1, :]
        out.append(total)
    return out


def mat_vec(a, f):
    parts = [a[k] * f[k : k + 1, :] for k in range(8)]
    while len(parts) > 1:
        parts = [parts[i] + parts[i + 1] for i in range(0, len(parts), 2)]
    return parts[0]


def mat_inv(t):
    t = list(t)
    sub = iota((8, 256), 0)
    for k in range(8):
        pivot = 1.0 / t[k][k : k + 1, :]
        column = t[k]
        at_k = sub == k
        for j in range(8):
            if j != k:
                row = t[j][k : k + 1, :] * pivot
                t[j] = jnp.where(at_k, row, t[j] - column * row)
        t[k] = jnp.where(at_k, pivot, -column * pivot)
    return t


def body(
    cond_hbm, mask_hbm, sidx_hbm, scur_hbm, gidx_hbm, out,
    cond, mask, sidx, scur, gidx, in_sem,
    mwin, side_r, side_l, diag, hsrc, winv3, e_east, e_south, kappa,
    s_a, s_b, v0, v1, w0, w1, lhs_g, lhs_s, cfac, clow, cup, mrow,
    ga0, gb0, ga1, gb1, ga2, gb2, ga3, gb3,
    nat, coef, halo_send, halo_recv, ga_send, ga_recv, gb_send, gb_recv,
):
    rho = lax.axis_index("row")
    col = lax.axis_index("col")
    gas = (ga0, ga1, ga2, ga3)
    gbs = (gb0, gb1, gb2, gb3)

    barrier = pltpu.get_barrier_semaphore()
    for i in range(1, N_COL):
        pl.semaphore_signal(barrier, inc=1, device_id=(rho, lax.rem(col + i, N_COL)), device_id_type=MESH)
    for i in range(1, N_ROW):
        pl.semaphore_signal(barrier, inc=1, device_id=(lax.rem(rho + i, N_ROW), col), device_id_type=MESH)
    diagonals = ((-1, -1), (-1, 1), (1, -1), (1, 1))

    def exists(dr, dc):
        ok = None
        for at, step, size in ((rho, dr, N_ROW), (col, dc, N_COL)):
            if step:
                here = (at > 0) if step < 0 else (at < size - 1)
                ok = here if ok is None else jnp.logical_and(ok, here)
        return ok

    for dr, dc in diagonals:
        @pl.when(exists(dr, dc))
        def _():
            pl.semaphore_signal(barrier, inc=1, device_id=(rho + dr, col + dc), device_id_type=MESH)

    fetches = [
        pltpu.make_async_copy(far, near, in_sem.at[n])
        for n, (far, near) in enumerate((
            (cond_hbm, cond), (mask_hbm, mask), (gidx_hbm, gidx), (sidx_hbm, sidx), (scur_hbm, scur),
        ))
    ]
    for fetch in fetches:
        fetch.start()
    for fetch in fetches:
        fetch.wait()
    mwin[MARGIN : MARGIN + CR, 0:CC] = cond[...] * mask[...].astype(F32)

    def land(dr, dc):
        rows = {-1: pl.ds(0, MARGIN), 0: pl.ds(MARGIN, CR), 1: pl.ds(MARGIN + CR, MARGIN)}[dr]
        if dc == 0:
            return mwin.at[rows, pl.ds(0, CC)]
        return (side_r if dc > 0 else side_l).at[rows, :]

    def take(dr, dc):
        rows = {-1: pl.ds(MARGIN, MARGIN), 0: pl.ds(MARGIN, CR), 1: pl.ds(MARGIN + CR - MARGIN, MARGIN)}[dr]
        cols = {-1: pl.ds(0, 128), 0: pl.ds(0, CC), 1: pl.ds(CC - 128, 128)}[dc]
        return mwin.at[rows, cols]

    around = [(dr, dc) for dr in (-1, 0, 1) for dc in (-1, 0, 1) if dr or dc]
    for dr, dc in around:
        @pl.when(jnp.logical_not(exists(dr, dc)))
        def _():
            ref = land(dr, dc)
            ref[...] = jnp.zeros(ref.shape, F32)

    def halo_copy(n, dr, dc):
        m = around.index((-dr, -dc))
        return pltpu.make_async_remote_copy(
            src_ref=take(dr, dc), dst_ref=land(-dr, -dc),
            send_sem=halo_send.at[n], recv_sem=halo_recv.at[m],
            device_id=(rho + dr, col + dc), device_id_type=MESH,
        )

    expected = N_COL - 1 + N_ROW - 1
    for dr, dc in diagonals:
        expected = expected + exists(dr, dc).astype(jnp.int32)
    pl.semaphore_wait(barrier, expected)

    for n, (dr, dc) in enumerate(around):
        @pl.when(exists(dr, dc))
        def _():
            halo_copy(n, dr, dc).start()

    gflat = flat_row(gidx[...].astype(F32)).astype(jnp.int32)
    sflat = flat_row(sidx[...].astype(F32)).astype(jnp.int32)
    cflat = flat_row(scur[...])
    g_row, g_col = gflat // NC, gflat % NC
    s_row, s_col = sflat // NC, sflat % NC

    own_b = iota((NB, 256), 1) // 16 == iota((NB, 256), 0)
    g_rel = g_row - rho * CR + MARGIN
    s_rel = s_row - rho * CR + MARGIN
    c_hi = cflat.astype(BF16).astype(F32)
    c_mid = (cflat - c_hi).astype(BF16).astype(F32)
    c_lo = cflat - c_hi - c_mid

    def build(r, carry):
        g_hit = jnp.logical_and(own_b, g_rel == r)
        s_hit = jnp.logical_and(own_b, s_rel == r)
        lhs_g[r] = jnp.where(g_hit, 1.0, 0.0).astype(BF16)
        lhs_s[r, :, 0:256] = jnp.where(s_hit, c_hi, 0.0).astype(BF16)
        lhs_s[r, :, 256:512] = jnp.where(s_hit, c_mid, 0.0).astype(BF16)
        lhs_s[r, :, 512:768] = jnp.where(s_hit, c_lo, 0.0).astype(BF16)
        return carry

    lax.fori_loop(0, WR, build, 0)

    def place(column):
        rel = column - col * CC
        return jnp.where(rel >= 576, -1, jnp.where(rel >= 0, rel, jnp.where(rel >= -64, rel + WC, -1)))

    spot = 5 * (iota((WC, 256), 0) % 128) + iota((WC, 256), 0) // 128
    g_hot = jnp.where(place(g_col) == spot, 1.0, 0.0).astype(BF16)
    s_one = jnp.where(place(s_col) == spot, 1.0, 0.0).astype(BF16)
    s_hot = jnp.concatenate([s_one, s_one, s_one], axis=1)

    STEP = 16

    def spread(i, carry):
        rows = pl.ds(i * STEP, STEP)
        diag[rows] = lax.dot_general(
            lhs_g[rows].reshape(STEP * NB, 256), g_hot, NT, preferred_element_type=F32
        ).reshape(STEP, NB, WC)
        hsrc[rows] = lax.dot_general(
            lhs_s[rows].reshape(STEP * NB, 768), s_hot, NT, preferred_element_type=F32
        ).reshape(STEP, NB, WC)
        return carry

    lax.fori_loop(0, WR // STEP, spread, 0)

    a1 = jnp.where(g_col // CC == iota((8, 256), 0), 1.0, 0.0).astype(BF16)
    a2 = jnp.where(
        jnp.logical_and(
            g_row // CR == iota((256, 256), 0) // 16,
            iota((256, 256), 1) // 16 == iota((256, 256), 0) % 16,
        ), 1.0, 0.0).astype(BF16)
    shunt_total = lax.dot_general(a1, a2, NT, preferred_element_type=F32)

    mrow[3, MARGIN : MARGIN + CR, :] = jnp.where(
        interleave(jnp.concatenate([mwin[MARGIN : MARGIN + CR, 0:CC], jnp.zeros((CR, 128), F32)], axis=1)) > 0.0,
        1.0, 0.0,
    )
    wide_zero = jnp.zeros((NB, WC), F32)
    inflow_acc = lax.fori_loop(
        MARGIN, MARGIN + CR, lambda r, acc: acc + hsrc[r] * mrow[3, pl.ds(r, 1), :], wide_zero, unroll=4
    )

    def total(field):
        return jnp.sum(jnp.sum(field, axis=0, keepdims=True), axis=1, keepdims=True)

    slot = iota((NB, 128), 1) // 16
    own_slot = slot == lax.rem(rho, 8)
    same_b = iota((NB, 128), 1) % 16 == iota((NB, 128), 0)
    row_slot = iota((1, 128), 1) // 16 == lax.rem(rho, 8)

    def one_row(value):
        return jnp.where(row_slot, jnp.broadcast_to(value, (1, 128)), 0.0)

    def b_row(acc, where):
        value = jnp.sum(acc, axis=1, keepdims=True)
        return jnp.sum(jnp.where(jnp.logical_and(where, same_b), value, 0.0), axis=0, keepdims=True)

    own_col = at_col() < CC

    def fold(x):
        parts = tiles(jnp.where(own_col, x, 0.0))
        return parts[0] + parts[1] + ((parts[2] + parts[3]) + parts[4])

    inflow_row = b_row(fold(inflow_acc), own_slot)

    for n, (dr, dc) in enumerate(around):
        @pl.when(exists(dr, dc))
        def _():
            halo_copy(n, dr, dc).wait_send()
            ref = land(dr, dc)
            pltpu.make_async_remote_copy(
                src_ref=ref, dst_ref=ref, send_sem=halo_send.at[n], recv_sem=halo_recv.at[n],
                device_id=(rho + dr, col + dc), device_id_type=MESH,
            ).wait_recv()
    lane = iota((WR, 128), 1)
    mwin[0:WR, CC:WC] = jnp.where(lane < 64, side_r[...], side_l[...])

    m = interleave(mwin[...])
    mrow[0] = m
    last = jnp.zeros((1, WC), F32)
    m_s = jnp.concatenate([mrow[0, 1:WR, :], last], axis=0)
    present = jnp.where(m > 0.0, 1.0, 0.0)
    present_s = jnp.where(m_s > 0.0, 1.0, 0.0)
    east = 0.5 * present * east_of(present) * (m + east_of(m))
    south = 0.5 * present * present_s * (m + m_s)
    west = west_of(east)
    mrow[0] = south
    north = jnp.concatenate([last, mrow[0, 0 : WR - 1, :]], axis=0)
    base = east + west + south + north + LEAKAGE
    mrow[1] = base
    mrow[2] = east
    mrow[3] = present
    at_r = iota((WR, WC), 0)
    at_c = jnp.broadcast_to(at_col(), (WR, WC))
    row_in = jnp.where(jnp.logical_and(at_r >= MARGIN, at_r < MARGIN + CR), 1.0, 0.0)
    row_in_s = jnp.where(jnp.logical_and(at_r >= MARGIN - 1, at_r < MARGIN + CR - 1), 1.0, 0.0)
    row_in_n = jnp.where(jnp.logical_and(at_r >= MARGIN + 1, at_r < MARGIN + CR + 1), 1.0, 0.0)
    col_in = jnp.where(at_c < CC, 1.0, 0.0)
    col_in_e = jnp.where(jnp.logical_or(at_c < CC - 1, at_c == WC - 1), 1.0, 0.0)
    col_in_w = jnp.where(jnp.logical_and(at_c >= 1, at_c <= CC), 1.0, 0.0)
    inside = row_in * col_in
    gap_field = ((((base - east) - west) - south) - north - LEAKAGE) * inside
    east_field = jnp.where(at_c == CC - 1, east * row_in, 0.0)
    south_field = jnp.where(at_r == MARGIN + CR - 1, south * col_in, 0.0)

    def put_natural(n, field, lo, hi, less=None):
        def step(r, carry):
            for half in range(2):
                sub = pl.ds(8 * half, 8)
                value = field[r + MARGIN, sub, :]
                if less is not None:
                    value = 81.0 * (value - less[8 * half : 8 * half + 8])
                nat[n, sub, r, :] = natural(tiles(value))
            return carry

        lax.fori_loop(lo, hi, step, 0, unroll=4)

    def send_a(g, rows):
        ga = gas[g]
        ga[rho] = jnp.concatenate(rows, axis=0)
        for i in range(1, N_ROW):
            pltpu.make_async_remote_copy(
                src_ref=ga.at[rho], dst_ref=ga.at[rho], send_sem=ga_send.at[g], recv_sem=ga_recv.at[g],
                device_id=(lax.rem(rho + i, N_ROW), col), device_id_type=MESH,
            ).start()

    def send_b(g):
        ga, gb = gas[g], gbs[g]
        peers = pl.ds(0, N_ROW - 1)
        pltpu.make_async_remote_copy(
            src_ref=ga.at[peers], dst_ref=ga.at[peers], send_sem=ga_send.at[g], recv_sem=ga_recv.at[g],
            device_id=(lax.rem(rho + 1, N_ROW), col), device_id_type=MESH,
        ).wait()
        for h in range(2):
            acc = ga[8 * h]
            for i in range(1, 8):
                acc = acc + ga[8 * h + i]
            gb[col, h] = acc
        for i in range(1, N_COL):
            pltpu.make_async_remote_copy(
                src_ref=gb.at[col], dst_ref=gb.at[col], send_sem=gb_send.at[g], recv_sem=gb_recv.at[g],
                device_id=(rho, lax.rem(col + i, N_COL)), device_id_type=MESH,
            ).start()

    def wait_b(g):
        gb = gbs[g]
        peers = pl.ds(0, N_COL - 1)
        pltpu.make_async_remote_copy(
            src_ref=gb.at[peers], dst_ref=gb.at[peers], send_sem=gb_send.at[g], recv_sem=gb_recv.at[g],
            device_id=(rho, lax.rem(col + 1, N_COL)), device_id_type=MESH,
        ).wait()

    def coarse(g, k):
        gb = gbs[g]
        return jnp.concatenate([gb[:, 0, k, :], gb[:, 1, k, :]], axis=1)

    send_a(0, [
        inflow_row, one_row(total(east_field)), one_row(total(south_field)), one_row(total(gap_field)),
    ])

    mrow[4] = (
        base * inside - east * (row_in * col_in_e) - west * (row_in * col_in_w)
        - south * (row_in_s * col_in) - north * (row_in_n * col_in)
    )
    mrow[5] = inside

    def coeffs(r, carry):
        rows = pl.ds(r, 1)
        shunt = diag[r]
        d = shunt + mrow[1, rows, :]
        inverse = 2.0 / d
        diag[r] = d
        winv3[r] = inverse
        kappa[r] = mrow[4, rows, :] + shunt * mrow[5, rows, :]
        here = hsrc[r] * mrow[3, rows, :]
        hsrc[r] = here
        v1[r] = (1.0 / 3.0) * inverse * here
        e_east[r] = jnp.broadcast_to(mrow[2, rows, :], (8, WC))
        e_south[r] = jnp.broadcast_to(mrow[0, rows, :], (8, WC))
        return carry

    lax.fori_loop(0, WR, coeffs, 0, unroll=2)

    def sweep(src, dst, width, extra=None, scale=None, image=None):
        rows = CR + 2 * width
        at_once = min(range(CHOICES[0], CHOICES[1]), key=lambda n: (-(-rows // n) * n, -n))
        count = -(-rows // at_once)
        lo = MARGIN - width - (count * at_once - rows) // 2

        def step(i, carry):
            r0 = lo + i * at_once
            for k in range(at_once):
                r = r0 + k
                e = tiles(e_east[r])
                south_here = tiles(e_south[r])
                south_north = tiles(e_south[r - 1])
                for half in range(2):
                    sub = pl.ds(8 * half, 8)
                    s = tiles(src[r, sub, :])
                    below = tiles(src[r + 1, sub, :])
                    above = tiles(src[r - 1, sub, :])
                    w3 = tiles(winv3[r, sub, :])
                    h = None if extra is None else tiles(extra[r, sub, :])
                    to_east = s[1:] + [roll(s[0], -1)]
                    flow = [e[j] * s[j] for j in range(4)]
                    to_west = [roll(e[4] * s[4], 1)] + flow
                    for j in range(5):
                        t = (e[j] * to_east[j] + to_west[j]) + (south_here[j] * below[j] + south_north[j] * above[j])
                        at = pl.ds(128 * j, 128)
                        if image is not None:
                            image[r, sub, at] = diag[r, sub, at] * s[j] - t
                        if dst is not None:
                            new = s[j] + w3[j] * t
                            if h is not None:
                                new = new + scale * h[j]
                            dst[r, sub, at] = new
            return carry

        lax.fori_loop(0, count, step, 0)

    def block_image(field):
        acc = lax.fori_loop(
            MARGIN - 1, MARGIN + CR + 1, lambda r, acc: acc + field[r] * kappa[r], wide_zero, unroll=2
        )
        parts = tiles(acc)
        return (parts[0] + parts[1]) + (parts[2] + parts[3]) + parts[4]

    def own_dots(*pairs):
        def step(r, accs):
            return tuple(acc + f[r] * g[r] for acc, (f, g) in zip(accs, pairs))

        accs = lax.fori_loop(MARGIN, MARGIN + CR, step, (wide_zero,) * len(pairs), unroll=2)
        return [fold(acc) for acc in accs]

    sweep(v1, s_a, 14, v1, 3.0)
    sweep(s_a, s_b, 13, v1, 9.0)
    sweep(s_b, s_a, 12, v1, 27.0)
    send_b(0)
    sweep(s_a, s_b, 11, v1, 81.0)
    ra = block_image(s_b) * (1.0 / 81.0)
    zero_row = jnp.zeros((1, 128), F32)
    send_a(1, [b_row(ra, own_slot), zero_row])
    ru = own_dots((s_b, hsrc))[0] * (1.0 / 81.0)

    put_natural(0, s_b, 0, EARLY)
    wait_b(0)
    f0 = coarse(0, 0)
    ec = coarse(0, 1)
    sc = coarse(0, 2)
    gap = coarse(0, 3)
    degree = LEAKAGE * CR * CC + shunt_total + ec + pltpu.roll(ec, 1, 0) + sc + roll(sc, 16)
    sub = iota((8, 256), 0)
    t = []
    for j in range(8):
        tj = jnp.where(sub == j, degree, 0.0)
        tj = jnp.where(sub == j - 1, -ec, tj)
        tj = jnp.where(sub == j + 1, -jnp.broadcast_to(ec[j : j + 1, :], (8, 256)), tj)
        t.append(tj)
    uvec = -sc
    lvec = roll(uvec, 16)
    x = mat_inv(t)
    for j in range(8):
        cfac[0, j] = x[j]
    ux = [uvec * x[j] for j in range(8)]
    lx = [lvec * x[j] for j in range(8)]
    p = [ux[j] * uvec[j : j + 1, :] for j in range(8)]
    q = [lx[j] * lvec[j : j + 1, :] for j in range(8)]
    w = [ux[j] * lvec[j : j + 1, :] for j in range(8)]
    wt = [lx[j] * uvec[j : j + 1, :] for j in range(8)]
    for level in range(1, 5):
        d = 16 << (level - 1)
        t = [t[j] - roll(p[j], d) - roll(q[j], -d) for j in range(8)]
        x = mat_inv(t)
        for j in range(8):
            cfac[level, j] = x[j]
        if level == 4:
            break
        low = [-roll(w[j], d) for j in range(8)]
        up = [-roll(wt[j], -d) for j in range(8)]
        low_t = [-roll(wt[j], d) for j in range(8)]
        up_t = [-roll(w[j], -d) for j in range(8)]
        for j in range(8):
            clow[level - 1, j] = low[j]
            cup[level - 1, j] = up[j]
        y = mat_mat(x, up)
        z = mat_mat(x, low)
        p = mat_mat(up_t, y)
        q = mat_mat(low_t, z)
        w = mat_mat(up_t, z)
        wt = mat_mat(low_t, y)

    def solve(f):
        h = mat_vec([cfac[0, j] for j in range(8)], f)
        f = f - lvec * roll(h, 16) - uvec * roll(h, -16)
        for level in range(1, 4):
            d = 16 << level
            h = mat_vec([cfac[level, j] for j in range(8)], f)
            f = f - mat_vec([clow[level - 1, j] for j in range(8)], roll(h, d))
            f = f - mat_vec([cup[level - 1, j] for j in range(8)], roll(h, -d))
        return mat_vec([cfac[4, j] for j in range(8)], f)

    wide_b = iota((NB, 256), 1) % 16 == iota((NB, 256), 0)

    def to_b(row):
        return jnp.sum(jnp.where(wide_b, row, 0.0), axis=1, keepdims=True)

    def dot_c(a, b):
        return to_b(jnp.sum(a * b, axis=0, keepdims=True))

    lane_c = jnp.broadcast_to(at_col(), (NB, WC))

    def around_field(y):
        fields = []
        lane_row = iota((8, 256), 1) // 16
        for dr in (-1, 0, 1):
            vals = []
            for dc in (0, 1, -1):
                hit = jnp.logical_and(lane_row == rho + dr, sub == col + dc)
                vals.append(to_b(jnp.sum(jnp.where(hit, y, 0.0), axis=0, keepdims=True)))
            fields.append(jnp.where(lane_c < CC, vals[0], jnp.where(lane_c < CC + 64, vals[1], vals[2])))
        return fields

    def combine(dst, src, fields, width, scale):
        spans = ((MARGIN - width, MARGIN), (MARGIN, MARGIN + CR), (MARGIN + CR, MARGIN + CR + width))
        for (lo, hi), field in zip(spans, fields):
            def step(r, carry):
                dst[r] = field + scale * src[r]
                return carry
            lax.fori_loop(lo, hi, step, 0, unroll=hi - lo if hi - lo < 16 else 4)

    y0 = solve(f0)
    combine(v0, s_b, around_field(y0), 11, 1.0 / 81.0)

    sweep(v0, s_a, 10, image=w0)
    send_b(1)
    sweep(s_a, s_b, 9)
    sweep(s_b, s_a, 8)
    sweep(s_a, s_b, 7)
    sweep(s_b, s_a, 6)
    ra0 = block_image(s_a) * (1.0 / 243.0)
    send_a(2, [b_row(ra0, own_slot), zero_row])
    wait_b(1)
    f1 = f0 + coarse(1, 0) + gap * y0
    g0 = solve(f1)
    combine(v1, s_a, around_field(g0), 6, -1.0 / 243.0)

    sweep(v1, s_b, 5, image=w1)
    sweep(s_b, s_a, 4)
    sweep(s_a, s_b, 3)
    sweep(s_b, s_a, 2)
    sweep(s_a, s_b, 1)
    mu0, mu1, mu2 = own_dots((v0, w0), (v1, w0), (v1, w1))
    sweep(s_b, None, 0, image=s_a)
    send_b(2)
    bab, bw1 = own_dots((s_b, s_a), (s_b, w1))
    bab = bab * (1.0 / (243.0 * 243.0))
    bw1 = bw1 * (1.0 / 243.0)
    ra1 = block_image(s_b) * (1.0 / 243.0)
    moments = zero_row
    for n, acc in enumerate((ru, mu0, mu1, mu2, bw1, bab)):
        moments = moments + b_row(acc, slot == n)
    send_a(3, [b_row(ra1, own_slot), moments])
    own_block = jnp.logical_and(iota((8, 256), 1) // 16 == rho, sub == col)

    def own_value(y):
        return to_b(jnp.sum(jnp.where(own_block, y, 0.0), axis=0, keepdims=True))

    y0_own = own_value(y0)
    put_natural(1, v1, 0, CR)
    wait_b(2)
    f2 = f1 - coarse(2, 0) + gap * g0
    g1 = solve(f2)
    put_natural(2, s_b, 0, CR // 2)
    send_b(3)
    put_natural(2, s_b, CR // 2, CR)
    put_natural(0, v0, EARLY, CR, jnp.broadcast_to(y0_own, (NB, WC)))
    g1_own = own_value(g1)
    energy_y = dot_c(f0, y0)
    g1w1 = dot_c(g1, f2)
    g1gap = dot_c(g1, g1 * gap)
    wait_b(3)
    ra1_all = coarse(3, 0)
    g1ra1 = dot_c(g1, ra1_all)
    mom = coarse(3, 1)
    mom = jnp.sum(mom[:, 0:128] + mom[:, 128:256], axis=0, keepdims=True)

    def moment(n):
        return jnp.sum(jnp.where(jnp.logical_and(slot == n, same_b), mom, 0.0), axis=1, keepdims=True)

    energy = moment(0) + energy_y
    m0, m1, m2 = moment(1), moment(2), moment(3)
    m3 = g1w1 - moment(4)
    m4 = g1w1 + g1gap - 2.0 * g1ra1 + moment(5)
    r1 = m0 - energy
    r2 = m1 - r1

    def ratio(a, b, scale):
        ok = b > scale
        return jnp.where(ok, a / jnp.where(ok, b, 1.0), 0.0)

    l10 = m1 / m0
    l20 = m2 / m0
    d1 = m2 - l10 * m1
    e21 = m3 - l20 * m1
    l21 = ratio(e21, d1, 0.0)
    d2 = m4 - l20 * m2 - l21 * e21
    t1 = r1 - l10 * energy
    t2 = r2 - l20 * energy - l21 * t1
    c2 = ratio(t2, d2, 0.0)
    c1 = ratio(t1, d1, 0.0) - l21 * c2
    c0 = energy / m0 - l10 * c1 - l20 * c2
    shift = c0 * y0_own + c2 * g1_own
    for n, c in enumerate((c0 * (1.0 / 81.0), c1, c2 * (-1.0 / 243.0), shift)):
        coef[n] = jnp.broadcast_to(c, (NB, CC))

    def finish(b, carry):
        w = [coef[n, pl.ds(b, 1), :] for n in range(4)]
        out[b] = w[0] * nat[0, b] + w[1] * nat[1, b] + (w[2] * nat[2, b] + w[3])
        return carry

    lax.fori_loop(0, NB, finish, 0)


def shards(conductance, nodata_mask, source_index, source_current, ground_index):
    big = pltpu.VMEM((WR, NB, WC), F32)
    edge = pltpu.VMEM((WR, 8, WC), F32)
    scratch = [
        pltpu.VMEM((CR, CC), F32), pltpu.VMEM((CR, CC), jnp.int32), pltpu.VMEM((NB, 16), jnp.int32),
        pltpu.VMEM((NB, 16), F32), pltpu.VMEM((NB, 16), jnp.int32), pltpu.SemaphoreType.DMA((5,)),
        pltpu.VMEM((WR, WC), F32), pltpu.VMEM((WR, 128), F32), pltpu.VMEM((WR, 128), F32),
        big, big, big, edge, edge, big,
        big, big, big, big, big, big,
        pltpu.VMEM((WR, NB, 256), BF16), pltpu.VMEM((WR, NB, 768), BF16),
        pltpu.VMEM((5, 8, 8, 256), F32), pltpu.VMEM((3, 8, 8, 256), F32), pltpu.VMEM((3, 8, 8, 256), F32),
        pltpu.VMEM((6, WR, WC), F32),
    ]
    for q in (4, 2, 2, 2):
        scratch += [pltpu.VMEM((N_ROW, q, 128), F32), pltpu.VMEM((N_COL, 2, q, 128), F32)]
    scratch += [pltpu.VMEM((3, NB, CR, CC), F32), pltpu.VMEM((4, NB, CC), F32)]
    scratch += [pltpu.SemaphoreType.DMA((8,)), pltpu.SemaphoreType.DMA((8,))]
    scratch += [pltpu.SemaphoreType.DMA((4,)) for _ in range(4)]
    return pl.pallas_call(
        body,
        out_shape=pltpu.VMEM((NB, CR, CC), F32),
        in_specs=[pl.BlockSpec(memory_space=pltpu.HBM)] * 5,
        out_specs=pl.BlockSpec(memory_space=pltpu.VMEM),
        scratch_shapes=scratch,
        compiler_params=pltpu.CompilerParams(
            collective_id=0, has_side_effects=True, vmem_limit_bytes=56 * 1024 * 1024
        ),
    )(conductance, nodata_mask, source_index, source_current, ground_index)


def solution(mesh):
    return jax.shard_map(
        shards,
        mesh=mesh,
        in_specs=(P("row", "col"), P("row", "col"), P(), P(), P()),
        out_specs=P(None, "row", "col"),
        check_vma=False,
    )
```

```python
import jax
import jax.numpy as jnp
from jax import lax
from jax.experimental import pallas as pl
from jax.experimental.pallas import tpu as pltpu
from jax.sharding import PartitionSpec as P

LEAKAGE = 0.0001
RELAXATION = 2.0 / 3.0
NB = 16
CR = 32
CC = 512
N_ROW = 16
N_COL = 8
NC = N_COL * CC
MARGIN = 16
EARLY = 16
CHOICES = (6, 12)
WR = CR + 2 * MARGIN
WC = CC + 128
F32 = jnp.float32
BF16 = jnp.bfloat16
MESH = pl.DeviceIdType.MESH
NT = (((1,), (1,)), ((), ()))


def iota(shape, dim):
    return lax.broadcasted_iota(jnp.int32, shape, dim)


def roll(x, shift):
    return pltpu.roll(x, shift % x.shape[-1], x.ndim - 1)


def at_col():
    c = iota((1, WC), 1)
    return 5 * (c % 128) + c // 128


def tiles(x):
    return [x[..., 128 * j : 128 * (j + 1)] for j in range(WC // 128)]


def east_of(x):
    t = tiles(x)
    return jnp.concatenate(t[1:] + [roll(t[0], -1)], axis=-1)


def west_of(x):
    t = tiles(x)
    return jnp.concatenate([roll(t[-1], 1)] + t[:-1], axis=-1)


def interleave(x):
    n = x.shape[0]
    lane = iota((n, 128), 1)
    source = tiles(x)
    out = []
    for j in range(5):
        p = 5 * lane + j
        part = None
        for t in range(5):
            got = jnp.take_along_axis(source[t], p % 128, axis=1)
            part = got if part is None else jnp.where(p // 128 == t, got, part)
        out.append(part)
    return jnp.concatenate(out, axis=1)


def natural(parts):
    n = parts[0].shape[0]
    lane = iota((n, 128), 1)
    out = []
    for t in range(CC // 128):
        c = 128 * t + lane
        fifth = (c * 52429) >> 18
        j_of = c - 5 * fifth
        tile = None
        for j in range(5):
            got = jnp.take_along_axis(parts[j], fifth, axis=1)
            tile = got if tile is None else jnp.where(j_of == j, got, tile)
        out.append(tile)
    return jnp.concatenate(out, axis=1)


def flat_row(x):
    pick = (iota((16, 256), 1) % 16 == iota((16, 256), 0)).astype(F32)
    tiled = jnp.dot(x, pick, precision=lax.Precision.HIGHEST, preferred_element_type=F32)
    own = iota((16, 256), 1) // 16 == iota((16, 256), 0)
    return jnp.sum(jnp.where(own, tiled, 0.0), axis=0, keepdims=True)


def mat_mat(a, b):
    out = []
    for j in range(8):
        total = a[0] * b[j][0:1, :]
        for k in range(1, 8):
            total = total + a[k] * b[j][k : k + 1, :]
        out.append(total)
    return out


def mat_vec(a, f):
    parts = [a[k] * f[k : k + 1, :] for k in range(8)]
    while len(parts) > 1:
        parts = [parts[i] + parts[i + 1] for i in range(0, len(parts), 2)]
    return parts[0]


def mat_inv(t):
    t = list(t)
    sub = iota((8, 256), 0)
    for k in range(8):
        pivot = 1.0 / t[k][k : k + 1, :]
        column = t[k]
        at_k = sub == k
        for j in range(8):
            if j != k:
                row = t[j][k : k + 1, :] * pivot
                t[j] = jnp.where(at_k, row, t[j] - column * row)
        t[k] = jnp.where(at_k, pivot, -column * pivot)
    return t


def body(
    cond_hbm, mask_hbm, sidx_hbm, scur_hbm, gidx_hbm, out,
    cond, mask, sidx, scur, gidx, in_sem,
    mwin, side_r, side_l, diag, hsrc, winv3, e_east, e_south, kappa,
    s_a, s_b, v0, v1, w0, w1, lhs_g, lhs_s, cfac, clow, cup, mrow,
    ga0, gb0, ga1, gb1, ga2, gb2, ga3, gb3,
    nat, coef, halo_send, halo_recv, ga_send, ga_recv, gb_send, gb_recv,
):
    rho = lax.axis_index("row")
    col = lax.axis_index("col")
    gas = (ga0, ga1, ga2, ga3)
    gbs = (gb0, gb1, gb2, gb3)

    barrier = pltpu.get_barrier_semaphore()
    for i in range(1, N_COL):
        pl.semaphore_signal(barrier, inc=1, device_id=(rho, lax.rem(col + i, N_COL)), device_id_type=MESH)
    for i in range(1, N_ROW):
        pl.semaphore_signal(barrier, inc=1, device_id=(lax.rem(rho + i, N_ROW), col), device_id_type=MESH)
    diagonals = ((-1, -1), (-1, 1), (1, -1), (1, 1))

    def exists(dr, dc):
        ok = None
        for at, step, size in ((rho, dr, N_ROW), (col, dc, N_COL)):
            if step:
                here = (at > 0) if step < 0 else (at < size - 1)
                ok = here if ok is None else jnp.logical_and(ok, here)
        return ok

    for dr, dc in diagonals:
        @pl.when(exists(dr, dc))
        def _():
            pl.semaphore_signal(barrier, inc=1, device_id=(rho + dr, col + dc), device_id_type=MESH)

    fetches = [
        pltpu.make_async_copy(far, near, in_sem.at[n])
        for n, (far, near) in enumerate((
            (cond_hbm, cond), (mask_hbm, mask), (gidx_hbm, gidx), (sidx_hbm, sidx), (scur_hbm, scur),
        ))
    ]
    for fetch in fetches:
        fetch.start()
    for fetch in fetches:
        fetch.wait()
    mwin[MARGIN : MARGIN + CR, 0:CC] = cond[...] * mask[...].astype(F32)

    near = ((-1, 0, 0), (1, 0, 0), (0, -1, 0), (0, 1, 0))
    far = ((-1, 0, 1), (1, 0, 1)) + tuple((dr, dc, 1) for dr, dc in diagonals)
    around = near + far

    def land(dr, dc, part):
        if dc == 0:
            first = (8 - 8 * part) if dr < 0 else MARGIN + CR + 8 * part
            return mwin.at[pl.ds(first, 8), pl.ds(0, CC)]
        rows = {-1: pl.ds(0, MARGIN), 0: pl.ds(MARGIN, CR), 1: pl.ds(MARGIN + CR, MARGIN)}[dr]
        return (side_r if dc > 0 else side_l).at[rows, :]

    def take(dr, dc, part):
        if dc == 0:
            first = (MARGIN + 8 * part) if dr < 0 else MARGIN + CR - 8 - 8 * part
            return mwin.at[pl.ds(first, 8), pl.ds(0, CC)]
        rows = {-1: pl.ds(MARGIN, MARGIN), 0: pl.ds(MARGIN, CR), 1: pl.ds(CR, MARGIN)}[dr]
        return mwin.at[rows, pl.ds(0, 128) if dc < 0 else pl.ds(CC - 128, 128)]

    for dr, dc, part in around:
        @pl.when(jnp.logical_not(exists(dr, dc)))
        def _():
            ref = land(dr, dc, part)
            ref[...] = jnp.zeros(ref.shape, F32)

    def halo_start(n):
        dr, dc, part = around[n]
        m = around.index((-dr, -dc, part))
        @pl.when(exists(dr, dc))
        def _():
            pltpu.make_async_remote_copy(
                src_ref=take(dr, dc, part), dst_ref=land(-dr, -dc, part),
                send_sem=halo_send.at[n], recv_sem=halo_recv.at[m],
                device_id=(rho + dr, col + dc), device_id_type=MESH,
            ).start()

    def halo_wait(n):
        dr, dc, part = around[n]
        @pl.when(exists(dr, dc))
        def _():
            pltpu.make_async_remote_copy(
                src_ref=take(dr, dc, part), dst_ref=land(dr, dc, part),
                send_sem=halo_send.at[n], recv_sem=halo_recv.at[n],
                device_id=(rho + dr, col + dc), device_id_type=MESH,
            ).wait()

    expected = N_COL - 1 + N_ROW - 1
    for dr, dc in diagonals:
        expected = expected + exists(dr, dc).astype(jnp.int32)
    pl.semaphore_wait(barrier, expected)

    for n in range(len(around)):
        halo_start(n)

    gflat = flat_row(gidx[...].astype(F32)).astype(jnp.int32)
    sflat = flat_row(sidx[...].astype(F32)).astype(jnp.int32)
    cflat = flat_row(scur[...])
    g_row, g_col = gflat // NC, gflat % NC
    s_row, s_col = sflat // NC, sflat % NC

    own_b = iota((NB, 256), 1) // 16 == iota((NB, 256), 0)
    g_rel = g_row - rho * CR + MARGIN
    s_rel = s_row - rho * CR + MARGIN
    c_hi = cflat.astype(BF16).astype(F32)
    c_mid = (cflat - c_hi).astype(BF16).astype(F32)
    c_lo = cflat - c_hi - c_mid

    def build(r, carry):
        g_hit = jnp.logical_and(own_b, g_rel == r)
        s_hit = jnp.logical_and(own_b, s_rel == r)
        lhs_g[r] = jnp.where(g_hit, 1.0, 0.0).astype(BF16)
        lhs_s[r, :, 0:256] = jnp.where(s_hit, c_hi, 0.0).astype(BF16)
        lhs_s[r, :, 256:512] = jnp.where(s_hit, c_mid, 0.0).astype(BF16)
        lhs_s[r, :, 512:768] = jnp.where(s_hit, c_lo, 0.0).astype(BF16)
        return carry

    lax.fori_loop(0, WR, build, 0, unroll=4)

    def place(column):
        rel = column - col * CC
        return jnp.where(rel >= 576, -1, jnp.where(rel >= 0, rel, jnp.where(rel >= -64, rel + WC, -1)))

    spot = 5 * (iota((WC, 256), 0) % 128) + iota((WC, 256), 0) // 128
    g_hot = jnp.where(place(g_col) == spot, 1.0, 0.0).astype(BF16)
    s_one = jnp.where(place(s_col) == spot, 1.0, 0.0).astype(BF16)
    s_hot = jnp.concatenate([s_one, s_one, s_one], axis=1)

    STEP = 32

    def spread(i, carry):
        rows = pl.ds(i * STEP, STEP)
        diag[rows] = lax.dot_general(
            lhs_g[rows].reshape(STEP * NB, 256), g_hot, NT, preferred_element_type=F32
        ).reshape(STEP, NB, WC)
        hsrc[rows] = lax.dot_general(
            lhs_s[rows].reshape(STEP * NB, 768), s_hot, NT, preferred_element_type=F32
        ).reshape(STEP, NB, WC)
        return carry

    lax.fori_loop(0, WR // STEP, spread, 0)

    a1 = jnp.where(g_col // CC == iota((8, 256), 0), 1.0, 0.0).astype(BF16)
    a2 = jnp.where(
        jnp.logical_and(
            g_row // CR == iota((256, 256), 0) // 16,
            iota((256, 256), 1) // 16 == iota((256, 256), 0) % 16,
        ), 1.0, 0.0).astype(BF16)
    shunt_total = lax.dot_general(a1, a2, NT, preferred_element_type=F32)

    mrow[3, MARGIN : MARGIN + CR, :] = jnp.where(
        interleave(jnp.concatenate([mwin[MARGIN : MARGIN + CR, 0:CC], jnp.zeros((CR, 128), F32)], axis=1)) > 0.0,
        1.0, 0.0,
    )
    wide_zero = jnp.zeros((NB, WC), F32)
    inflow_acc = lax.fori_loop(
        MARGIN, MARGIN + CR, lambda r, acc: acc + hsrc[r] * mrow[3, pl.ds(r, 1), :], wide_zero, unroll=4
    )

    def total(field):
        return jnp.sum(jnp.sum(field, axis=0, keepdims=True), axis=1, keepdims=True)

    slot = iota((NB, 128), 1) // 16
    own_slot = slot == lax.rem(rho, 8)
    same_b = iota((NB, 128), 1) % 16 == iota((NB, 128), 0)
    row_slot = iota((1, 128), 1) // 16 == lax.rem(rho, 8)

    def one_row(value):
        return jnp.where(row_slot, jnp.broadcast_to(value, (1, 128)), 0.0)

    def b_row(acc, where):
        value = jnp.sum(acc, axis=1, keepdims=True)
        return jnp.sum(jnp.where(jnp.logical_and(where, same_b), value, 0.0), axis=0, keepdims=True)

    own_col = at_col() < CC

    def fold(x):
        parts = tiles(jnp.where(own_col, x, 0.0))
        return parts[0] + parts[1] + ((parts[2] + parts[3]) + parts[4])

    inflow_row = b_row(fold(inflow_acc), own_slot)

    def put_natural(n, field, lo, hi, less=None):
        def step(r, carry):
            for half in range(2):
                sub = pl.ds(8 * half, 8)
                value = field[r + MARGIN, sub, :]
                if less is not None:
                    value = 81.0 * (value - less[8 * half : 8 * half + 8])
                nat[n, sub, r, :] = natural(tiles(value))
            return carry

        lax.fori_loop(lo, hi, step, 0, unroll=4)

    def send_a(g, rows):
        ga = gas[g]
        ga[rho] = jnp.concatenate(rows, axis=0)
        for i in range(1, N_ROW):
            pltpu.make_async_remote_copy(
                src_ref=ga.at[rho], dst_ref=ga.at[rho], send_sem=ga_send.at[g], recv_sem=ga_recv.at[g],
                device_id=(lax.rem(rho + i, N_ROW), col), device_id_type=MESH,
            ).start()

    def send_b(g):
        ga, gb = gas[g], gbs[g]
        peers = pl.ds(0, N_ROW - 1)
        pltpu.make_async_remote_copy(
            src_ref=ga.at[peers], dst_ref=ga.at[peers], send_sem=ga_send.at[g], recv_sem=ga_recv.at[g],
            device_id=(lax.rem(rho + 1, N_ROW), col), device_id_type=MESH,
        ).wait()
        for h in range(2):
            acc = ga[8 * h]
            for i in range(1, 8):
                acc = acc + ga[8 * h + i]
            gb[col, h] = acc
        for i in range(1, N_COL):
            pltpu.make_async_remote_copy(
                src_ref=gb.at[col], dst_ref=gb.at[col], send_sem=gb_send.at[g], recv_sem=gb_recv.at[g],
                device_id=(rho, lax.rem(col + i, N_COL)), device_id_type=MESH,
            ).start()

    def wait_b(g):
        gb = gbs[g]
        peers = pl.ds(0, N_COL - 1)
        pltpu.make_async_remote_copy(
            src_ref=gb.at[peers], dst_ref=gb.at[peers], send_sem=gb_send.at[g], recv_sem=gb_recv.at[g],
            device_id=(rho, lax.rem(col + 1, N_COL)), device_id_type=MESH,
        ).wait()

    def coarse(g, k):
        gb = gbs[g]
        return jnp.concatenate([gb[:, 0, k, :], gb[:, 1, k, :]], axis=1)

    for n in range(len(near)):
        halo_wait(n)
    inner = slice(MARGIN, MARGIN + CR)
    lane = iota((WR, 128), 1)
    beside = jnp.where(lane[0:CR] < 64, side_r[inner, :], side_l[inner, :])
    m = jnp.concatenate([mwin[inner, 0:CC], beside], axis=1)

    def held_of(x):
        return jnp.where(x > 0.0, 1.0, 0.0)

    present = held_of(m)
    east = 0.5 * present * roll(present, -1) * (m + roll(m, -1))
    west = roll(east, 1)[:, 0:CC]
    east = east[:, 0:CC]
    m, present = m[:, 0:CC], present[:, 0:CC]
    m_s, m_n = mwin[MARGIN + 1 : MARGIN + CR + 1, 0:CC], mwin[MARGIN - 1 : MARGIN + CR - 1, 0:CC]
    south = 0.5 * present * held_of(m_s) * (m + m_s)
    north = 0.5 * held_of(m_n) * present * (m_n + m)
    base = east + west + south + north + LEAKAGE
    gap_total = total((((base - east) - west) - south) - north - LEAKAGE)
    east_total = jnp.sum(east[:, CC - 1 : CC], axis=0, keepdims=True)
    south_total = jnp.sum(south[CR - 1 : CR, :], axis=1, keepdims=True)
    send_a(0, [inflow_row, one_row(east_total), one_row(south_total), one_row(gap_total)])

    for n in range(len(near), len(around)):
        halo_wait(n)
    mwin[0:WR, CC:WC] = jnp.where(lane < 64, side_r[...], side_l[...])

    m = interleave(mwin[...])
    mrow[0] = m
    last = jnp.zeros((1, WC), F32)
    m_s = jnp.concatenate([mrow[0, 1:WR, :], last], axis=0)
    present = jnp.where(m > 0.0, 1.0, 0.0)
    present_s = jnp.where(m_s > 0.0, 1.0, 0.0)
    east = 0.5 * present * east_of(present) * (m + east_of(m))
    south = 0.5 * present * present_s * (m + m_s)
    west = west_of(east)
    mrow[0] = south
    north = jnp.concatenate([last, mrow[0, 0 : WR - 1, :]], axis=0)
    base = east + west + south + north + LEAKAGE
    mrow[1] = base
    mrow[2] = east
    mrow[3] = present
    at_r = iota((WR, WC), 0)
    at_c = jnp.broadcast_to(at_col(), (WR, WC))
    row_in = jnp.where(jnp.logical_and(at_r >= MARGIN, at_r < MARGIN + CR), 1.0, 0.0)
    row_in_s = jnp.where(jnp.logical_and(at_r >= MARGIN - 1, at_r < MARGIN + CR - 1), 1.0, 0.0)
    row_in_n = jnp.where(jnp.logical_and(at_r >= MARGIN + 1, at_r < MARGIN + CR + 1), 1.0, 0.0)
    col_in = jnp.where(at_c < CC, 1.0, 0.0)
    col_in_e = jnp.where(jnp.logical_or(at_c < CC - 1, at_c == WC - 1), 1.0, 0.0)
    col_in_w = jnp.where(jnp.logical_and(at_c >= 1, at_c <= CC), 1.0, 0.0)
    inside = row_in * col_in

    mrow[4] = (
        base * inside - east * (row_in * col_in_e) - west * (row_in * col_in_w)
        - south * (row_in_s * col_in) - north * (row_in_n * col_in)
    )
    mrow[5] = inside

    def coeffs(r, inner):
        rows = pl.ds(r, 1)
        shunt = diag[r]
        d = shunt + mrow[1, rows, :]
        inverse = 2.0 / d
        here = hsrc[r] * mrow[3, rows, :]
        winv3[r] = inverse
        v1[r] = (1.0 / 3.0) * inverse * here
        e_east[r] = jnp.broadcast_to(mrow[2, rows, :], (8, WC))
        e_south[r] = jnp.broadcast_to(mrow[0, rows, :], (8, WC))
        if inner:
            diag[r] = d
            hsrc[r] = here
            kappa[r] = mrow[4, rows, :] + shunt * mrow[5, rows, :]

    def coeffs_rim(i, carry):
        coeffs(1 + i, False)
        coeffs(MARGIN + CR + i, False)
        return carry

    def coeffs_block(i, carry):
        coeffs(MARGIN + 2 * i, True)
        coeffs(MARGIN + 2 * i + 1, True)
        return carry

    e_south[0] = jnp.broadcast_to(mrow[0, 0:1, :], (8, WC))
    lax.fori_loop(0, MARGIN - 1, coeffs_rim, 0)
    lax.fori_loop(0, CR // 2, coeffs_block, 0)
    for r in (MARGIN - 1, MARGIN + CR):
        kappa[r] = jnp.broadcast_to(mrow[4, r : r + 1, :], (NB, WC))

    def sweep(src, dst, width, extra=None, scale=None, image=None):
        rows = CR + 2 * width
        at_once = min(range(CHOICES[0], CHOICES[1]), key=lambda n: (-(-rows // n) * n, -n))
        count = -(-rows // at_once)
        lo = MARGIN - width - (count * at_once - rows) // 2

        def step(i, carry):
            r0 = lo + i * at_once
            for k in range(at_once):
                r = r0 + k
                e = tiles(e_east[r])
                south_here = tiles(e_south[r])
                south_north = tiles(e_south[r - 1])
                for half in range(2):
                    sub = pl.ds(8 * half, 8)
                    s = tiles(src[r, sub, :])
                    below = tiles(src[r + 1, sub, :])
                    above = tiles(src[r - 1, sub, :])
                    w3 = tiles(winv3[r, sub, :])
                    h = None if extra is None else tiles(extra[r, sub, :])
                    to_east = s[1:] + [roll(s[0], -1)]
                    flow = [e[j] * s[j] for j in range(4)]
                    to_west = [roll(e[4] * s[4], 1)] + flow
                    for j in range(5):
                        t = (e[j] * to_east[j] + to_west[j]) + (south_here[j] * below[j] + south_north[j] * above[j])
                        at = pl.ds(128 * j, 128)
                        if image is not None:
                            image[r, sub, at] = diag[r, sub, at] * s[j] - t
                        if dst is not None:
                            new = s[j] + w3[j] * t
                            if h is not None:
                                new = new + scale * h[j]
                            dst[r, sub, at] = new
            return carry

        lax.fori_loop(0, count, step, 0)

    def block_image(field):
        acc = lax.fori_loop(
            MARGIN - 1, MARGIN + CR + 1, lambda r, acc: acc + field[r] * kappa[r], wide_zero, unroll=2
        )
        parts = tiles(acc)
        return (parts[0] + parts[1]) + (parts[2] + parts[3]) + parts[4]

    def own_dots(*pairs):
        def step(r, accs):
            return tuple(acc + f[r] * g[r] for acc, (f, g) in zip(accs, pairs))

        accs = lax.fori_loop(MARGIN, MARGIN + CR, step, (wide_zero,) * len(pairs), unroll=2)
        return [fold(acc) for acc in accs]

    sweep(v1, s_a, 14, v1, 3.0)
    sweep(s_a, s_b, 13, v1, 9.0)
    sweep(s_b, s_a, 12, v1, 27.0)
    send_b(0)
    sweep(s_a, s_b, 11, v1, 81.0)
    ra = block_image(s_b) * (1.0 / 81.0)
    zero_row = jnp.zeros((1, 128), F32)
    send_a(1, [b_row(ra, own_slot), zero_row])
    ru = own_dots((s_b, hsrc))[0] * (1.0 / 81.0)

    put_natural(0, s_b, 0, EARLY)
    wait_b(0)
    f0 = coarse(0, 0)
    ec = coarse(0, 1)
    sc = coarse(0, 2)
    gap = coarse(0, 3)
    degree = LEAKAGE * CR * CC + shunt_total + ec + pltpu.roll(ec, 1, 0) + sc + roll(sc, 16)
    sub = iota((8, 256), 0)
    t = []
    for j in range(8):
        tj = jnp.where(sub == j, degree, 0.0)
        tj = jnp.where(sub == j - 1, -ec, tj)
        tj = jnp.where(sub == j + 1, -jnp.broadcast_to(ec[j : j + 1, :], (8, 256)), tj)
        t.append(tj)
    uvec = -sc
    lvec = roll(uvec, 16)
    x = mat_inv(t)
    for j in range(8):
        cfac[0, j] = x[j]
    ux = [uvec * x[j] for j in range(8)]
    lx = [lvec * x[j] for j in range(8)]
    p = [ux[j] * uvec[j : j + 1, :] for j in range(8)]
    q = [lx[j] * lvec[j : j + 1, :] for j in range(8)]
    w = [ux[j] * lvec[j : j + 1, :] for j in range(8)]
    wt = [lx[j] * uvec[j : j + 1, :] for j in range(8)]
    for level in range(1, 5):
        d = 16 << (level - 1)
        t = [t[j] - roll(p[j], d) - roll(q[j], -d) for j in range(8)]
        x = mat_inv(t)
        for j in range(8):
            cfac[level, j] = x[j]
        if level == 4:
            break
        low = [-roll(w[j], d) for j in range(8)]
        up = [-roll(wt[j], -d) for j in range(8)]
        low_t = [-roll(wt[j], d) for j in range(8)]
        up_t = [-roll(w[j], -d) for j in range(8)]
        for j in range(8):
            clow[level - 1, j] = low[j]
            cup[level - 1, j] = up[j]
        y = mat_mat(x, up)
        z = mat_mat(x, low)
        p = mat_mat(up_t, y)
        q = mat_mat(low_t, z)
        w = mat_mat(up_t, z)
        wt = mat_mat(low_t, y)

    def solve(f):
        h = mat_vec([cfac[0, j] for j in range(8)], f)
        f = f - lvec * roll(h, 16) - uvec * roll(h, -16)
        for level in range(1, 4):
            d = 16 << level
            h = mat_vec([cfac[level, j] for j in range(8)], f)
            f = f - mat_vec([clow[level - 1, j] for j in range(8)], roll(h, d))
            f = f - mat_vec([cup[level - 1, j] for j in range(8)], roll(h, -d))
        return mat_vec([cfac[4, j] for j in range(8)], f)

    wide_b = iota((NB, 256), 1) % 16 == iota((NB, 256), 0)

    def to_b(row):
        return jnp.sum(jnp.where(wide_b, row, 0.0), axis=1, keepdims=True)

    def dot_c(a, b):
        return to_b(jnp.sum(a * b, axis=0, keepdims=True))

    lane_c = jnp.broadcast_to(at_col(), (NB, WC))

    def around_field(y):
        fields = []
        lane_row = iota((8, 256), 1) // 16
        for dr in (-1, 0, 1):
            vals = []
            for dc in (0, 1, -1):
                hit = jnp.logical_and(lane_row == rho + dr, sub == col + dc)
                vals.append(to_b(jnp.sum(jnp.where(hit, y, 0.0), axis=0, keepdims=True)))
            fields.append(jnp.where(lane_c < CC, vals[0], jnp.where(lane_c < CC + 64, vals[1], vals[2])))
        return fields

    def combine(dst, src, fields, width, scale):
        spans = ((MARGIN - width, MARGIN), (MARGIN, MARGIN + CR), (MARGIN + CR, MARGIN + CR + width))
        for (lo, hi), field in zip(spans, fields):
            def step(r, carry):
                dst[r] = field + scale * src[r]
                return carry
            lax.fori_loop(lo, hi, step, 0, unroll=hi - lo if hi - lo < 16 else 4)

    y0 = solve(f0)
    combine(v0, s_b, around_field(y0), 11, 1.0 / 81.0)

    sweep(v0, s_a, 10, image=w0)
    send_b(1)
    sweep(s_a, s_b, 9)
    sweep(s_b, s_a, 8)
    sweep(s_a, s_b, 7)
    sweep(s_b, s_a, 6)
    ra0 = block_image(s_a) * (1.0 / 243.0)
    send_a(2, [b_row(ra0, own_slot), zero_row])
    (mu0,) = own_dots((v0, w0))
    wait_b(1)
    f1 = f0 + coarse(1, 0) + gap * y0
    g0 = solve(f1)
    combine(v1, s_a, around_field(g0), 6, -1.0 / 243.0)

    sweep(v1, s_b, 5, image=w1)
    sweep(s_b, s_a, 4)
    sweep(s_a, s_b, 3)
    sweep(s_b, s_a, 2)
    sweep(s_a, s_b, 1)
    mu1, mu2 = own_dots((v1, w0), (v1, w1))
    sweep(s_b, None, 0, image=s_a)
    send_b(2)
    bab, bw1 = own_dots((s_b, s_a), (s_b, w1))
    bab = bab * (1.0 / (243.0 * 243.0))
    bw1 = bw1 * (1.0 / 243.0)
    ra1 = block_image(s_b) * (1.0 / 243.0)
    moments = zero_row
    for n, acc in enumerate((ru, mu0, mu1, mu2, bw1, bab)):
        moments = moments + b_row(acc, slot == n)
    send_a(3, [b_row(ra1, own_slot), moments])
    own_block = jnp.logical_and(iota((8, 256), 1) // 16 == rho, sub == col)

    def own_value(y):
        return to_b(jnp.sum(jnp.where(own_block, y, 0.0), axis=0, keepdims=True))

    y0_own = own_value(y0)
    put_natural(1, v1, 0, CR)
    wait_b(2)
    f2 = f1 - coarse(2, 0) + gap * g0
    g1 = solve(f2)
    put_natural(2, s_b, 0, CR // 2)
    send_b(3)
    put_natural(2, s_b, CR // 2, CR)
    put_natural(0, v0, EARLY, CR, jnp.broadcast_to(y0_own, (NB, WC)))
    g1_own = own_value(g1)
    energy_y = dot_c(f0, y0)
    g1w1 = dot_c(g1, f2)
    g1gap = dot_c(g1, g1 * gap)
    wait_b(3)
    ra1_all = coarse(3, 0)
    g1ra1 = dot_c(g1, ra1_all)
    mom = coarse(3, 1)
    mom = jnp.sum(mom[:, 0:128] + mom[:, 128:256], axis=0, keepdims=True)

    def moment(n):
        return jnp.sum(jnp.where(jnp.logical_and(slot == n, same_b), mom, 0.0), axis=1, keepdims=True)

    energy = moment(0) + energy_y
    m0, m1, m2 = moment(1), moment(2), moment(3)
    m3 = g1w1 - moment(4)
    m4 = g1w1 + g1gap - 2.0 * g1ra1 + moment(5)
    r1 = m0 - energy
    r2 = m1 - r1

    def ratio(a, b, scale):
        ok = b > scale
        return jnp.where(ok, a / jnp.where(ok, b, 1.0), 0.0)

    l10 = m1 / m0
    l20 = m2 / m0
    d1 = m2 - l10 * m1
    e21 = m3 - l20 * m1
    l21 = ratio(e21, d1, 0.0)
    d2 = m4 - l20 * m2 - l21 * e21
    t1 = r1 - l10 * energy
    t2 = r2 - l20 * energy - l21 * t1
    c2 = ratio(t2, d2, 0.0)
    c1 = ratio(t1, d1, 0.0) - l21 * c2
    c0 = energy / m0 - l10 * c1 - l20 * c2
    shift = c0 * y0_own + c2 * g1_own
    for n, c in enumerate((c0 * (1.0 / 81.0), c1, c2 * (-1.0 / 243.0), shift)):
        coef[n] = jnp.broadcast_to(c, (NB, CC))

    def finish(b, carry):
        w = [coef[n, pl.ds(b, 1), :] for n in range(4)]
        out[b] = w[0] * nat[0, b] + w[1] * nat[1, b] + (w[2] * nat[2, b] + w[3])
        return carry

    lax.fori_loop(0, NB, finish, 0)


def shards(conductance, nodata_mask, source_index, source_current, ground_index):
    big = pltpu.VMEM((WR, NB, WC), F32)
    edge = pltpu.VMEM((WR, 8, WC), F32)
    scratch = [
        pltpu.VMEM((CR, CC), F32), pltpu.VMEM((CR, CC), jnp.int32), pltpu.VMEM((NB, 16), jnp.int32),
        pltpu.VMEM((NB, 16), F32), pltpu.VMEM((NB, 16), jnp.int32), pltpu.SemaphoreType.DMA((5,)),
        pltpu.VMEM((WR, WC), F32), pltpu.VMEM((WR, 128), F32), pltpu.VMEM((WR, 128), F32),
        big, big, big, edge, edge, big,
        big, big, big, big, big, big,
        pltpu.VMEM((WR, NB, 256), BF16), pltpu.VMEM((WR, NB, 768), BF16),
        pltpu.VMEM((5, 8, 8, 256), F32), pltpu.VMEM((3, 8, 8, 256), F32), pltpu.VMEM((3, 8, 8, 256), F32),
        pltpu.VMEM((6, WR, WC), F32),
    ]
    for q in (4, 2, 2, 2):
        scratch += [pltpu.VMEM((N_ROW, q, 128), F32), pltpu.VMEM((N_COL, 2, q, 128), F32)]
    scratch += [pltpu.VMEM((3, NB, CR, CC), F32), pltpu.VMEM((4, NB, CC), F32)]
    scratch += [pltpu.SemaphoreType.DMA((10,)), pltpu.SemaphoreType.DMA((10,))]
    scratch += [pltpu.SemaphoreType.DMA((4,)) for _ in range(4)]
    return pl.pallas_call(
        body,
        out_shape=pltpu.VMEM((NB, CR, CC), F32),
        in_specs=[pl.BlockSpec(memory_space=pltpu.HBM)] * 5,
        out_specs=pl.BlockSpec(memory_space=pltpu.VMEM),
        scratch_shapes=scratch,
        compiler_params=pltpu.CompilerParams(
            collective_id=0, has_side_effects=True, vmem_limit_bytes=56 * 1024 * 1024
        ),
    )(conductance, nodata_mask, source_index, source_current, ground_index)


def solution(mesh):
    return jax.shard_map(
        shards,
        mesh=mesh,
        in_specs=(P("row", "col"), P("row", "col"), P(), P(), P()),
        out_specs=P(None, "row", "col"),
        check_vma=False,
    )
```

```python
import jax
import jax.numpy as jnp
from jax import lax
from jax.experimental import pallas as pl
from jax.experimental.pallas import tpu as pltpu
from jax.sharding import PartitionSpec as P

LEAKAGE = 0.0001
RELAXATION = 2.0 / 3.0
NB = 16
CR = 32
CC = 512
N_ROW = 16
N_COL = 8
NC = N_COL * CC
MARGIN = 16
EARLY = 16
CHOICES = (6, 12)
WR = CR + 2 * MARGIN
WC = CC + 128
F32 = jnp.float32
BF16 = jnp.bfloat16
MESH = pl.DeviceIdType.MESH
NT = (((1,), (1,)), ((), ()))


def iota(shape, dim):
    return lax.broadcasted_iota(jnp.int32, shape, dim)


def roll(x, shift):
    return pltpu.roll(x, shift % x.shape[-1], x.ndim - 1)


def at_col():
    c = iota((1, WC), 1)
    return 5 * (c % 128) + c // 128


def tiles(x):
    return [x[..., 128 * j : 128 * (j + 1)] for j in range(WC // 128)]


def east_of(x):
    t = tiles(x)
    return jnp.concatenate(t[1:] + [roll(t[0], -1)], axis=-1)


def west_of(x):
    t = tiles(x)
    return jnp.concatenate([roll(t[-1], 1)] + t[:-1], axis=-1)


def interleave(x):
    n = x.shape[0]
    lane = iota((n, 128), 1)
    source = tiles(x)
    out = []
    for j in range(5):
        p = 5 * lane + j
        part = None
        for t in range(5):
            got = jnp.take_along_axis(source[t], p % 128, axis=1)
            part = got if part is None else jnp.where(p // 128 == t, got, part)
        out.append(part)
    return jnp.concatenate(out, axis=1)


def natural(parts):
    n = parts[0].shape[0]
    lane = iota((n, 128), 1)
    out = []
    for t in range(CC // 128):
        c = 128 * t + lane
        fifth = (c * 52429) >> 18
        j_of = c - 5 * fifth
        tile = None
        for j in range(5):
            got = jnp.take_along_axis(parts[j], fifth, axis=1)
            tile = got if tile is None else jnp.where(j_of == j, got, tile)
        out.append(tile)
    return jnp.concatenate(out, axis=1)


def flat_row(x):
    pick = (iota((16, 256), 1) % 16 == iota((16, 256), 0)).astype(F32)
    tiled = jnp.dot(x, pick, precision=lax.Precision.HIGHEST, preferred_element_type=F32)
    own = iota((16, 256), 1) // 16 == iota((16, 256), 0)
    return jnp.sum(jnp.where(own, tiled, 0.0), axis=0, keepdims=True)


def mat_mat(a, b):
    out = []
    for j in range(8):
        total = a[0] * b[j][0:1, :]
        for k in range(1, 8):
            total = total + a[k] * b[j][k : k + 1, :]
        out.append(total)
    return out


def mat_vec(a, f):
    parts = [a[k] * f[k : k + 1, :] for k in range(8)]
    while len(parts) > 1:
        parts = [parts[i] + parts[i + 1] for i in range(0, len(parts), 2)]
    return parts[0]


def mat_inv(t):
    t = list(t)
    sub = iota((8, 256), 0)
    for k in range(8):
        pivot = 1.0 / t[k][k : k + 1, :]
        column = t[k]
        at_k = sub == k
        for j in range(8):
            if j != k:
                row = t[j][k : k + 1, :] * pivot
                t[j] = jnp.where(at_k, row, t[j] - column * row)
        t[k] = jnp.where(at_k, pivot, -column * pivot)
    return t


def body(
    cond_hbm, mask_hbm, sidx_hbm, scur_hbm, gidx_hbm, out,
    cond, mask, sidx, scur, gidx, in_sem,
    mwin, side_r, side_l, diag, hsrc, winv3, e_east, e_south, kappa,
    s_a, s_b, v0, v1, w0, w1, lhs_g, lhs_s, cfac, clow, cup, mrow,
    ga0, gb0, ga1, gb1, ga2, gb2, ga3, gb3,
    nat, coef, halo_send, halo_recv, ga_send, ga_recv, gb_send, gb_recv,
):
    rho = lax.axis_index("row")
    col = lax.axis_index("col")
    gas = (ga0, ga1, ga2, ga3)
    gbs = (gb0, gb1, gb2, gb3)

    barrier = pltpu.get_barrier_semaphore()
    for i in range(1, N_COL):
        pl.semaphore_signal(barrier, inc=1, device_id=(rho, lax.rem(col + i, N_COL)), device_id_type=MESH)
    for i in range(1, N_ROW):
        pl.semaphore_signal(barrier, inc=1, device_id=(lax.rem(rho + i, N_ROW), col), device_id_type=MESH)
    diagonals = ((-1, -1), (-1, 1), (1, -1), (1, 1))

    def exists(dr, dc):
        ok = None
        for at, step, size in ((rho, dr, N_ROW), (col, dc, N_COL)):
            if step:
                here = (at > 0) if step < 0 else (at < size - 1)
                ok = here if ok is None else jnp.logical_and(ok, here)
        return ok

    for dr, dc in diagonals:
        @pl.when(exists(dr, dc))
        def _():
            pl.semaphore_signal(barrier, inc=1, device_id=(rho + dr, col + dc), device_id_type=MESH)

    fetches = [
        pltpu.make_async_copy(far, near, in_sem.at[n])
        for n, (far, near) in enumerate((
            (cond_hbm, cond), (mask_hbm, mask), (gidx_hbm, gidx), (sidx_hbm, sidx), (scur_hbm, scur),
        ))
    ]
    for fetch in fetches:
        fetch.start()
    for fetch in fetches:
        fetch.wait()
    mwin[MARGIN : MARGIN + CR, 0:CC] = cond[...] * mask[...].astype(F32)

    near = ((-1, 0, 0), (1, 0, 0), (0, -1, 0), (0, 1, 0))
    far = ((-1, 0, 1), (1, 0, 1)) + tuple((dr, dc, 1) for dr, dc in diagonals)
    around = near + far

    def land(dr, dc, part):
        if dc == 0:
            first = (8 - 8 * part) if dr < 0 else MARGIN + CR + 8 * part
            return mwin.at[pl.ds(first, 8), pl.ds(0, CC)]
        rows = {-1: pl.ds(0, MARGIN), 0: pl.ds(MARGIN, CR), 1: pl.ds(MARGIN + CR, MARGIN)}[dr]
        return (side_r if dc > 0 else side_l).at[rows, :]

    def take(dr, dc, part):
        if dc == 0:
            first = (MARGIN + 8 * part) if dr < 0 else MARGIN + CR - 8 - 8 * part
            return mwin.at[pl.ds(first, 8), pl.ds(0, CC)]
        rows = {-1: pl.ds(MARGIN, MARGIN), 0: pl.ds(MARGIN, CR), 1: pl.ds(CR, MARGIN)}[dr]
        return mwin.at[rows, pl.ds(0, 128) if dc < 0 else pl.ds(CC - 128, 128)]

    for dr, dc, part in around:
        @pl.when(jnp.logical_not(exists(dr, dc)))
        def _():
            ref = land(dr, dc, part)
            ref[...] = jnp.zeros(ref.shape, F32)

    def halo_start(n):
        dr, dc, part = around[n]
        m = around.index((-dr, -dc, part))
        @pl.when(exists(dr, dc))
        def _():
            pltpu.make_async_remote_copy(
                src_ref=take(dr, dc, part), dst_ref=land(-dr, -dc, part),
                send_sem=halo_send.at[n], recv_sem=halo_recv.at[m],
                device_id=(rho + dr, col + dc), device_id_type=MESH,
            ).start()

    def halo_wait(n):
        dr, dc, part = around[n]
        @pl.when(exists(dr, dc))
        def _():
            pltpu.make_async_remote_copy(
                src_ref=take(dr, dc, part), dst_ref=land(dr, dc, part),
                send_sem=halo_send.at[n], recv_sem=halo_recv.at[n],
                device_id=(rho + dr, col + dc), device_id_type=MESH,
            ).wait()

    expected = N_COL - 1 + N_ROW - 1
    for dr, dc in diagonals:
        expected = expected + exists(dr, dc).astype(jnp.int32)
    pl.semaphore_wait(barrier, expected)

    for n in range(len(around)):
        halo_start(n)

    gflat = flat_row(gidx[...].astype(F32)).astype(jnp.int32)
    sflat = flat_row(sidx[...].astype(F32)).astype(jnp.int32)
    cflat = flat_row(scur[...])
    g_row, g_col = gflat // NC, gflat % NC
    s_row, s_col = sflat // NC, sflat % NC

    own_b = iota((NB, 256), 1) // 16 == iota((NB, 256), 0)
    g_rel = g_row - rho * CR + MARGIN
    s_rel = s_row - rho * CR + MARGIN
    c_hi = cflat.astype(BF16).astype(F32)
    c_mid = (cflat - c_hi).astype(BF16).astype(F32)
    c_lo = cflat - c_hi - c_mid

    def build(r, carry):
        g_hit = jnp.logical_and(own_b, g_rel == r)
        s_hit = jnp.logical_and(own_b, s_rel == r)
        lhs_g[r] = jnp.where(g_hit, 1.0, 0.0).astype(BF16)
        lhs_s[r, :, 0:256] = jnp.where(s_hit, c_hi, 0.0).astype(BF16)
        lhs_s[r, :, 256:512] = jnp.where(s_hit, c_mid, 0.0).astype(BF16)
        lhs_s[r, :, 512:768] = jnp.where(s_hit, c_lo, 0.0).astype(BF16)
        return carry

    lax.fori_loop(0, WR, build, 0, unroll=4)

    def place(column):
        rel = column - col * CC
        return jnp.where(rel >= 576, -1, jnp.where(rel >= 0, rel, jnp.where(rel >= -64, rel + WC, -1)))

    spot = 5 * (iota((WC, 256), 0) % 128) + iota((WC, 256), 0) // 128
    g_hot = jnp.where(place(g_col) == spot, 1.0, 0.0).astype(BF16)
    s_one = jnp.where(place(s_col) == spot, 1.0, 0.0).astype(BF16)
    s_hot = jnp.concatenate([s_one, s_one, s_one], axis=1)

    STEP = 32

    def spread(i, carry):
        rows = pl.ds(i * STEP, STEP)
        diag[rows] = lax.dot_general(
            lhs_g[rows].reshape(STEP * NB, 256), g_hot, NT, preferred_element_type=F32
        ).reshape(STEP, NB, WC)
        hsrc[rows] = lax.dot_general(
            lhs_s[rows].reshape(STEP * NB, 768), s_hot, NT, preferred_element_type=F32
        ).reshape(STEP, NB, WC)
        return carry

    lax.fori_loop(0, WR // STEP, spread, 0)

    a1 = jnp.where(g_col // CC == iota((8, 256), 0), 1.0, 0.0).astype(BF16)
    a2 = jnp.where(
        jnp.logical_and(
            g_row // CR == iota((256, 256), 0) // 16,
            iota((256, 256), 1) // 16 == iota((256, 256), 0) % 16,
        ), 1.0, 0.0).astype(BF16)
    shunt_total = lax.dot_general(a1, a2, NT, preferred_element_type=F32)

    mrow[3, MARGIN : MARGIN + CR, :] = jnp.where(
        interleave(jnp.concatenate([mwin[MARGIN : MARGIN + CR, 0:CC], jnp.zeros((CR, 128), F32)], axis=1)) > 0.0,
        1.0, 0.0,
    )
    wide_zero = jnp.zeros((NB, WC), F32)
    inflow_acc = lax.fori_loop(
        MARGIN, MARGIN + CR, lambda r, acc: acc + hsrc[r] * mrow[3, pl.ds(r, 1), :], wide_zero, unroll=4
    )

    def total(field):
        return jnp.sum(jnp.sum(field, axis=0, keepdims=True), axis=1, keepdims=True)

    slot = iota((NB, 128), 1) // 16
    own_slot = slot == lax.rem(rho, 8)
    same_b = iota((NB, 128), 1) % 16 == iota((NB, 128), 0)
    row_slot = iota((1, 128), 1) // 16 == lax.rem(rho, 8)

    def one_row(value):
        return jnp.where(row_slot, jnp.broadcast_to(value, (1, 128)), 0.0)

    def b_row(acc, where):
        value = jnp.sum(acc, axis=1, keepdims=True)
        return jnp.sum(jnp.where(jnp.logical_and(where, same_b), value, 0.0), axis=0, keepdims=True)

    own_col = at_col() < CC

    def fold(x):
        parts = tiles(jnp.where(own_col, x, 0.0))
        return parts[0] + parts[1] + ((parts[2] + parts[3]) + parts[4])

    inflow_row = b_row(fold(inflow_acc), own_slot)

    def put_natural(n, field, lo, hi, less=None):
        def step(r, carry):
            for half in range(2):
                sub = pl.ds(8 * half, 8)
                value = field[r + MARGIN, sub, :]
                if less is not None:
                    value = 81.0 * (value - less[8 * half : 8 * half + 8])
                nat[n, sub, r, :] = natural(tiles(value))
            return carry

        lax.fori_loop(lo, hi, step, 0, unroll=4)

    def ring(d):
        return min(d, 4 - d)

    slow, fast = rho // 4, lax.rem(rho, 4)
    row_steps = sorted(((a, b) for a in range(4) for b in range(4) if a or b), key=lambda t: -ring(t[0]) - ring(t[1]))
    row_peers = [lax.rem(slow + a, 4) * 4 + lax.rem(fast + b, 4) for a, b in row_steps]
    chip, core = col // 2, lax.rem(col, 2)
    col_steps = sorted(((a, b) for a in range(4) for b in range(2) if a or b), key=lambda t: (-ring(t[0]), -t[1]))
    col_peers = [lax.rem(chip + a, 4) * 2 + lax.rem(core + b, 2) for a, b in col_steps]

    def send_a(g, rows):
        ga = gas[g]
        ga[rho] = jnp.concatenate(rows, axis=0)
        for peer in row_peers:
            pltpu.make_async_remote_copy(
                src_ref=ga.at[rho], dst_ref=ga.at[rho], send_sem=ga_send.at[g], recv_sem=ga_recv.at[g],
                device_id=(peer, col), device_id_type=MESH,
            ).start()

    def send_b(g):
        ga, gb = gas[g], gbs[g]
        peers = pl.ds(0, N_ROW - 1)
        pltpu.make_async_remote_copy(
            src_ref=ga.at[peers], dst_ref=ga.at[peers], send_sem=ga_send.at[g], recv_sem=ga_recv.at[g],
            device_id=(lax.rem(rho + 1, N_ROW), col), device_id_type=MESH,
        ).wait()
        for h in range(2):
            acc = ga[8 * h]
            for i in range(1, 8):
                acc = acc + ga[8 * h + i]
            gb[col, h] = acc
        for peer in col_peers:
            pltpu.make_async_remote_copy(
                src_ref=gb.at[col], dst_ref=gb.at[col], send_sem=gb_send.at[g], recv_sem=gb_recv.at[g],
                device_id=(rho, peer), device_id_type=MESH,
            ).start()

    def wait_b(g):
        gb = gbs[g]
        peers = pl.ds(0, N_COL - 1)
        pltpu.make_async_remote_copy(
            src_ref=gb.at[peers], dst_ref=gb.at[peers], send_sem=gb_send.at[g], recv_sem=gb_recv.at[g],
            device_id=(rho, lax.rem(col + 1, N_COL)), device_id_type=MESH,
        ).wait()

    def coarse(g, k):
        gb = gbs[g]
        return jnp.concatenate([gb[:, 0, k, :], gb[:, 1, k, :]], axis=1)

    for n in range(len(near)):
        halo_wait(n)
    inner = slice(MARGIN, MARGIN + CR)
    lane = iota((WR, 128), 1)
    beside = jnp.where(lane[0:CR] < 64, side_r[inner, :], side_l[inner, :])
    m = jnp.concatenate([mwin[inner, 0:CC], beside], axis=1)

    def held_of(x):
        return jnp.where(x > 0.0, 1.0, 0.0)

    present = held_of(m)
    east = 0.5 * present * roll(present, -1) * (m + roll(m, -1))
    west = roll(east, 1)[:, 0:CC]
    east = east[:, 0:CC]
    m, present = m[:, 0:CC], present[:, 0:CC]
    m_s, m_n = mwin[MARGIN + 1 : MARGIN + CR + 1, 0:CC], mwin[MARGIN - 1 : MARGIN + CR - 1, 0:CC]
    south = 0.5 * present * held_of(m_s) * (m + m_s)
    north = 0.5 * held_of(m_n) * present * (m_n + m)
    base = east + west + south + north + LEAKAGE
    gap_total = total((((base - east) - west) - south) - north - LEAKAGE)
    east_total = jnp.sum(east[:, CC - 1 : CC], axis=0, keepdims=True)
    south_total = jnp.sum(south[CR - 1 : CR, :], axis=1, keepdims=True)
    send_a(0, [inflow_row, one_row(east_total), one_row(south_total), one_row(gap_total)])

    for n in range(len(near), len(around)):
        halo_wait(n)
    mwin[0:WR, CC:WC] = jnp.where(lane < 64, side_r[...], side_l[...])

    m = interleave(mwin[...])
    mrow[0] = m
    last = jnp.zeros((1, WC), F32)
    m_s = jnp.concatenate([mrow[0, 1:WR, :], last], axis=0)
    present = jnp.where(m > 0.0, 1.0, 0.0)
    present_s = jnp.where(m_s > 0.0, 1.0, 0.0)
    east = 0.5 * present * east_of(present) * (m + east_of(m))
    south = 0.5 * present * present_s * (m + m_s)
    west = west_of(east)
    mrow[0] = south
    north = jnp.concatenate([last, mrow[0, 0 : WR - 1, :]], axis=0)
    base = east + west + south + north + LEAKAGE
    mrow[1] = base
    mrow[2] = east
    mrow[3] = present
    at_r = iota((WR, WC), 0)
    at_c = jnp.broadcast_to(at_col(), (WR, WC))
    row_in = jnp.where(jnp.logical_and(at_r >= MARGIN, at_r < MARGIN + CR), 1.0, 0.0)
    row_in_s = jnp.where(jnp.logical_and(at_r >= MARGIN - 1, at_r < MARGIN + CR - 1), 1.0, 0.0)
    row_in_n = jnp.where(jnp.logical_and(at_r >= MARGIN + 1, at_r < MARGIN + CR + 1), 1.0, 0.0)
    col_in = jnp.where(at_c < CC, 1.0, 0.0)
    col_in_e = jnp.where(jnp.logical_or(at_c < CC - 1, at_c == WC - 1), 1.0, 0.0)
    col_in_w = jnp.where(jnp.logical_and(at_c >= 1, at_c <= CC), 1.0, 0.0)
    inside = row_in * col_in

    mrow[4] = (
        base * inside - east * (row_in * col_in_e) - west * (row_in * col_in_w)
        - south * (row_in_s * col_in) - north * (row_in_n * col_in)
    )
    mrow[5] = inside

    def coeffs(r, inner):
        rows = pl.ds(r, 1)
        shunt = diag[r]
        d = shunt + mrow[1, rows, :]
        inverse = 2.0 / d
        here = hsrc[r] * mrow[3, rows, :]
        winv3[r] = inverse
        v1[r] = (1.0 / 3.0) * inverse * here
        e_east[r] = jnp.broadcast_to(mrow[2, rows, :], (8, WC))
        e_south[r] = jnp.broadcast_to(mrow[0, rows, :], (8, WC))
        if inner:
            diag[r] = d
            hsrc[r] = here
            kappa[r] = mrow[4, rows, :] + shunt * mrow[5, rows, :]

    def coeffs_rim(i, carry):
        coeffs(1 + i, False)
        coeffs(MARGIN + CR + i, False)
        return carry

    def coeffs_block(i, carry):
        coeffs(MARGIN + 2 * i, True)
        coeffs(MARGIN + 2 * i + 1, True)
        return carry

    e_south[0] = jnp.broadcast_to(mrow[0, 0:1, :], (8, WC))
    lax.fori_loop(0, MARGIN - 1, coeffs_rim, 0)
    lax.fori_loop(0, CR // 2, coeffs_block, 0)
    for r in (MARGIN - 1, MARGIN + CR):
        kappa[r] = jnp.broadcast_to(mrow[4, r : r + 1, :], (NB, WC))

    def sweep(src, dst, width, extra=None, scale=None, image=None):
        rows = CR + 2 * width
        at_once = min(range(CHOICES[0], CHOICES[1]), key=lambda n: (-(-rows // n) * n, -n))
        count = -(-rows // at_once)
        lo = MARGIN - width - (count * at_once - rows) // 2

        def step(i, carry):
            r0 = lo + i * at_once
            for k in range(at_once):
                r = r0 + k
                e = tiles(e_east[r])
                south_here = tiles(e_south[r])
                south_north = tiles(e_south[r - 1])
                for half in range(2):
                    sub = pl.ds(8 * half, 8)
                    s = tiles(src[r, sub, :])
                    below = tiles(src[r + 1, sub, :])
                    above = tiles(src[r - 1, sub, :])
                    w3 = tiles(winv3[r, sub, :])
                    h = None if extra is None else tiles(extra[r, sub, :])
                    to_east = s[1:] + [roll(s[0], -1)]
                    flow = [e[j] * s[j] for j in range(4)]
                    to_west = [roll(e[4] * s[4], 1)] + flow
                    for j in range(5):
                        t = (e[j] * to_east[j] + to_west[j]) + (south_here[j] * below[j] + south_north[j] * above[j])
                        at = pl.ds(128 * j, 128)
                        if image is not None:
                            image[r, sub, at] = diag[r, sub, at] * s[j] - t
                        if dst is not None:
                            new = s[j] + w3[j] * t
                            if h is not None:
                                new = new + scale * h[j]
                            dst[r, sub, at] = new
            return carry

        lax.fori_loop(0, count, step, 0)

    def block_image(field):
        acc = lax.fori_loop(
            MARGIN - 1, MARGIN + CR + 1, lambda r, acc: acc + field[r] * kappa[r], wide_zero, unroll=2
        )
        parts = tiles(acc)
        return (parts[0] + parts[1]) + (parts[2] + parts[3]) + parts[4]

    def own_dots(*pairs):
        def step(r, accs):
            return tuple(acc + f[r] * g[r] for acc, (f, g) in zip(accs, pairs))

        accs = lax.fori_loop(MARGIN, MARGIN + CR, step, (wide_zero,) * len(pairs), unroll=4)
        return [fold(acc) for acc in accs]

    sweep(v1, s_a, 14, v1, 3.0)
    sweep(s_a, s_b, 13, v1, 9.0)
    sweep(s_b, s_a, 12, v1, 27.0)
    send_b(0)
    sweep(s_a, s_b, 11, v1, 81.0)
    ra = block_image(s_b) * (1.0 / 81.0)
    zero_row = jnp.zeros((1, 128), F32)
    send_a(1, [b_row(ra, own_slot), zero_row])
    ru = own_dots((s_b, hsrc))[0] * (1.0 / 81.0)

    put_natural(0, s_b, 0, EARLY)
    wait_b(0)
    f0 = coarse(0, 0)
    ec = coarse(0, 1)
    sc = coarse(0, 2)
    gap = coarse(0, 3)
    degree = LEAKAGE * CR * CC + shunt_total + ec + pltpu.roll(ec, 1, 0) + sc + roll(sc, 16)
    sub = iota((8, 256), 0)
    t = []
    for j in range(8):
        tj = jnp.where(sub == j, degree, 0.0)
        tj = jnp.where(sub == j - 1, -ec, tj)
        tj = jnp.where(sub == j + 1, -jnp.broadcast_to(ec[j : j + 1, :], (8, 256)), tj)
        t.append(tj)
    uvec = -sc
    lvec = roll(uvec, 16)
    x = mat_inv(t)
    for j in range(8):
        cfac[0, j] = x[j]
    ux = [uvec * x[j] for j in range(8)]
    lx = [lvec * x[j] for j in range(8)]
    p = [ux[j] * uvec[j : j + 1, :] for j in range(8)]
    q = [lx[j] * lvec[j : j + 1, :] for j in range(8)]
    w = [ux[j] * lvec[j : j + 1, :] for j in range(8)]
    wt = [lx[j] * uvec[j : j + 1, :] for j in range(8)]
    for level in range(1, 5):
        d = 16 << (level - 1)
        t = [t[j] - roll(p[j], d) - roll(q[j], -d) for j in range(8)]
        x = mat_inv(t)
        for j in range(8):
            cfac[level, j] = x[j]
        if level == 4:
            break
        low = [-roll(w[j], d) for j in range(8)]
        up = [-roll(wt[j], -d) for j in range(8)]
        low_t = [-roll(wt[j], d) for j in range(8)]
        up_t = [-roll(w[j], -d) for j in range(8)]
        for j in range(8):
            clow[level - 1, j] = low[j]
            cup[level - 1, j] = up[j]
        y = mat_mat(x, up)
        z = mat_mat(x, low)
        p = mat_mat(up_t, y)
        q = mat_mat(low_t, z)
        w = mat_mat(up_t, z)
        wt = mat_mat(low_t, y)

    def solve(f):
        h = mat_vec([cfac[0, j] for j in range(8)], f)
        f = f - lvec * roll(h, 16) - uvec * roll(h, -16)
        for level in range(1, 4):
            d = 16 << level
            h = mat_vec([cfac[level, j] for j in range(8)], f)
            f = f - mat_vec([clow[level - 1, j] for j in range(8)], roll(h, d))
            f = f - mat_vec([cup[level - 1, j] for j in range(8)], roll(h, -d))
        return mat_vec([cfac[4, j] for j in range(8)], f)

    wide_b = iota((NB, 256), 1) % 16 == iota((NB, 256), 0)

    def to_b(row):
        return jnp.sum(jnp.where(wide_b, row, 0.0), axis=1, keepdims=True)

    def dot_c(a, b):
        return to_b(jnp.sum(a * b, axis=0, keepdims=True))

    lane_c = jnp.broadcast_to(at_col(), (NB, WC))

    def around_field(y):
        fields = []
        lane_row = iota((8, 256), 1) // 16
        for dr in (-1, 0, 1):
            vals = []
            for dc in (0, 1, -1):
                hit = jnp.logical_and(lane_row == rho + dr, sub == col + dc)
                vals.append(to_b(jnp.sum(jnp.where(hit, y, 0.0), axis=0, keepdims=True)))
            fields.append(jnp.where(lane_c < CC, vals[0], jnp.where(lane_c < CC + 64, vals[1], vals[2])))
        return fields

    def combine(dst, src, fields, width, scale):
        spans = ((MARGIN - width, MARGIN), (MARGIN, MARGIN + CR), (MARGIN + CR, MARGIN + CR + width))
        for (lo, hi), field in zip(spans, fields):
            def step(r, carry):
                dst[r] = field + scale * src[r]
                return carry
            lax.fori_loop(lo, hi, step, 0, unroll=hi - lo if hi - lo < 16 else 4)

    y0 = solve(f0)
    combine(v0, s_b, around_field(y0), 11, 1.0 / 81.0)

    sweep(v0, s_a, 10, image=w0)
    send_b(1)
    sweep(s_a, s_b, 9)
    sweep(s_b, s_a, 8)
    sweep(s_a, s_b, 7)
    sweep(s_b, s_a, 6)
    ra0 = block_image(s_a) * (1.0 / 243.0)
    send_a(2, [b_row(ra0, own_slot), zero_row])
    (mu0,) = own_dots((v0, w0))
    wait_b(1)
    f1 = f0 + coarse(1, 0) + gap * y0
    g0 = solve(f1)
    combine(v1, s_a, around_field(g0), 6, -1.0 / 243.0)

    sweep(v1, s_b, 5, image=w1)
    sweep(s_b, s_a, 4)
    sweep(s_a, s_b, 3)
    sweep(s_b, s_a, 2)
    sweep(s_a, s_b, 1)
    mu1, mu2 = own_dots((v1, w0), (v1, w1))
    sweep(s_b, None, 0, image=s_a)
    send_b(2)
    bab, bw1 = own_dots((s_b, s_a), (s_b, w1))
    bab = bab * (1.0 / (243.0 * 243.0))
    bw1 = bw1 * (1.0 / 243.0)
    ra1 = block_image(s_b) * (1.0 / 243.0)
    moments = zero_row
    for n, acc in enumerate((ru, mu0, mu1, mu2, bw1, bab)):
        moments = moments + b_row(acc, slot == n)
    send_a(3, [b_row(ra1, own_slot), moments])
    own_block = jnp.logical_and(iota((8, 256), 1) // 16 == rho, sub == col)

    def own_value(y):
        return to_b(jnp.sum(jnp.where(own_block, y, 0.0), axis=0, keepdims=True))

    y0_own = own_value(y0)
    put_natural(1, v1, 0, CR)
    wait_b(2)
    f2 = f1 - coarse(2, 0) + gap * g0
    g1 = solve(f2)
    put_natural(2, s_b, 0, CR // 2)
    send_b(3)
    put_natural(2, s_b, CR // 2, CR)
    put_natural(0, v0, EARLY, CR, jnp.broadcast_to(y0_own, (NB, WC)))
    g1_own = own_value(g1)
    energy_y = dot_c(f0, y0)
    g1w1 = dot_c(g1, f2)
    g1gap = dot_c(g1, g1 * gap)
    wait_b(3)
    ra1_all = coarse(3, 0)
    g1ra1 = dot_c(g1, ra1_all)
    mom = coarse(3, 1)
    mom = jnp.sum(mom[:, 0:128] + mom[:, 128:256], axis=0, keepdims=True)

    def moment(n):
        return jnp.sum(jnp.where(jnp.logical_and(slot == n, same_b), mom, 0.0), axis=1, keepdims=True)

    energy = moment(0) + energy_y
    m0, m1, m2 = moment(1), moment(2), moment(3)
    m3 = g1w1 - moment(4)
    m4 = g1w1 + g1gap - 2.0 * g1ra1 + moment(5)
    r1 = m0 - energy
    r2 = m1 - r1

    def ratio(a, b, scale):
        ok = b > scale
        return jnp.where(ok, a / jnp.where(ok, b, 1.0), 0.0)

    l10 = m1 / m0
    l20 = m2 / m0
    d1 = m2 - l10 * m1
    e21 = m3 - l20 * m1
    l21 = ratio(e21, d1, 0.0)
    d2 = m4 - l20 * m2 - l21 * e21
    t1 = r1 - l10 * energy
    t2 = r2 - l20 * energy - l21 * t1
    c2 = ratio(t2, d2, 0.0)
    c1 = ratio(t1, d1, 0.0) - l21 * c2
    c0 = energy / m0 - l10 * c1 - l20 * c2
    shift = c0 * y0_own + c2 * g1_own
    for n, c in enumerate((c0 * (1.0 / 81.0), c1, c2 * (-1.0 / 243.0), shift)):
        coef[n] = jnp.broadcast_to(c, (NB, CC))

    def finish(b, carry):
        w = [coef[n, pl.ds(b, 1), :] for n in range(4)]
        out[b] = w[0] * nat[0, b] + w[1] * nat[1, b] + (w[2] * nat[2, b] + w[3])
        return carry

    lax.fori_loop(0, NB, finish, 0, unroll=2)


def shards(conductance, nodata_mask, source_index, source_current, ground_index):
    big = pltpu.VMEM((WR, NB, WC), F32)
    edge = pltpu.VMEM((WR, 8, WC), F32)
    scratch = [
        pltpu.VMEM((CR, CC), F32), pltpu.VMEM((CR, CC), jnp.int32), pltpu.VMEM((NB, 16), jnp.int32),
        pltpu.VMEM((NB, 16), F32), pltpu.VMEM((NB, 16), jnp.int32), pltpu.SemaphoreType.DMA((5,)),
        pltpu.VMEM((WR, WC), F32), pltpu.VMEM((WR, 128), F32), pltpu.VMEM((WR, 128), F32),
        big, big, big, edge, edge, big,
        big, big, big, big, big, big,
        pltpu.VMEM((WR, NB, 256), BF16), pltpu.VMEM((WR, NB, 768), BF16),
        pltpu.VMEM((5, 8, 8, 256), F32), pltpu.VMEM((3, 8, 8, 256), F32), pltpu.VMEM((3, 8, 8, 256), F32),
        pltpu.VMEM((6, WR, WC), F32),
    ]
    for q in (4, 2, 2, 2):
        scratch += [pltpu.VMEM((N_ROW, q, 128), F32), pltpu.VMEM((N_COL, 2, q, 128), F32)]
    scratch += [pltpu.VMEM((3, NB, CR, CC), F32), pltpu.VMEM((4, NB, CC), F32)]
    scratch += [pltpu.SemaphoreType.DMA((10,)), pltpu.SemaphoreType.DMA((10,))]
    scratch += [pltpu.SemaphoreType.DMA((4,)) for _ in range(4)]
    return pl.pallas_call(
        body,
        out_shape=pltpu.VMEM((NB, CR, CC), F32),
        in_specs=[pl.BlockSpec(memory_space=pltpu.HBM)] * 5,
        out_specs=pl.BlockSpec(memory_space=pltpu.VMEM),
        scratch_shapes=scratch,
        compiler_params=pltpu.CompilerParams(
            collective_id=0, has_side_effects=True, vmem_limit_bytes=56 * 1024 * 1024
        ),
    )(conductance, nodata_mask, source_index, source_current, ground_index)


def solution(mesh):
    return jax.shard_map(
        shards,
        mesh=mesh,
        in_specs=(P("row", "col"), P("row", "col"), P(), P(), P()),
        out_specs=P(None, "row", "col"),
        check_vma=False,
    )
```

```python
import jax
import jax.numpy as jnp
from jax import lax
from jax.experimental import pallas as pl
from jax.experimental.pallas import tpu as pltpu
from jax.sharding import PartitionSpec as P

LEAKAGE = 0.0001
RELAXATION = 2.0 / 3.0
NB = 16
CR = 32
CC = 512
N_ROW = 16
N_COL = 8
NC = N_COL * CC
MARGIN = 16
EARLY = 16
CHOICES = (6, 12)
WR = CR + 2 * MARGIN
WC = CC + 128
F32 = jnp.float32
BF16 = jnp.bfloat16
MESH = pl.DeviceIdType.MESH
NT = (((1,), (1,)), ((), ()))


def iota(shape, dim):
    return lax.broadcasted_iota(jnp.int32, shape, dim)


def roll(x, shift):
    return pltpu.roll(x, shift % x.shape[-1], x.ndim - 1)


def at_col():
    c = iota((1, WC), 1)
    return 5 * (c % 128) + c // 128


def tiles(x):
    return [x[..., 128 * j : 128 * (j + 1)] for j in range(WC // 128)]


def east_of(x):
    t = tiles(x)
    return jnp.concatenate(t[1:] + [roll(t[0], -1)], axis=-1)


def west_of(x):
    t = tiles(x)
    return jnp.concatenate([roll(t[-1], 1)] + t[:-1], axis=-1)


def interleave(x):
    n = x.shape[0]
    lane = iota((n, 128), 1)
    source = tiles(x)
    out = []
    for j in range(5):
        p = 5 * lane + j
        part = None
        for t in range(5):
            got = jnp.take_along_axis(source[t], p % 128, axis=1)
            part = got if part is None else jnp.where(p // 128 == t, got, part)
        out.append(part)
    return jnp.concatenate(out, axis=1)


def natural(parts):
    n = parts[0].shape[0]
    lane = iota((n, 128), 1)
    out = []
    for t in range(CC // 128):
        c = 128 * t + lane
        fifth = (c * 52429) >> 18
        j_of = c - 5 * fifth
        tile = None
        for j in range(5):
            got = jnp.take_along_axis(parts[j], fifth, axis=1)
            tile = got if tile is None else jnp.where(j_of == j, got, tile)
        out.append(tile)
    return jnp.concatenate(out, axis=1)


def flat_row(x):
    pick = (iota((16, 256), 1) % 16 == iota((16, 256), 0)).astype(F32)
    tiled = jnp.dot(x, pick, precision=lax.Precision.HIGHEST, preferred_element_type=F32)
    own = iota((16, 256), 1) // 16 == iota((16, 256), 0)
    return jnp.sum(jnp.where(own, tiled, 0.0), axis=0, keepdims=True)


def mat_mat(a, b):
    out = []
    for j in range(8):
        total = a[0] * b[j][0:1, :]
        for k in range(1, 8):
            total = total + a[k] * b[j][k : k + 1, :]
        out.append(total)
    return out


def mat_vec(a, f):
    parts = [a[k] * f[k : k + 1, :] for k in range(8)]
    while len(parts) > 1:
        parts = [parts[i] + parts[i + 1] for i in range(0, len(parts), 2)]
    return parts[0]


def mat_inv(t):
    t = list(t)
    sub = iota((8, 256), 0)
    for k in range(8):
        pivot = 1.0 / t[k][k : k + 1, :]
        column = t[k]
        at_k = sub == k
        for j in range(8):
            if j != k:
                row = t[j][k : k + 1, :] * pivot
                t[j] = jnp.where(at_k, row, t[j] - column * row)
        t[k] = jnp.where(at_k, pivot, -column * pivot)
    return t


def body(
    cond_hbm, mask_hbm, sidx_hbm, scur_hbm, gidx_hbm, out,
    cond, mask, sidx, scur, gidx, in_sem,
    mwin, side_r, side_l, diag, hsrc, winv3, e_east, e_south, kappa,
    s_a, s_b, v0, v1, w0, w1, lhs_g, lhs_s, cfac, clow, cup, mrow,
    ga0, gb0, ga1, gb1, ga2, gb2, ga3, gb3,
    nat, coef, halo_send, halo_recv, ga_send, ga_recv, gb_send, gb_recv,
):
    rho = lax.axis_index("row")
    col = lax.axis_index("col")
    gas = (ga0, ga1, ga2, ga3)
    gbs = (gb0, gb1, gb2, gb3)

    barrier = pltpu.get_barrier_semaphore()
    for i in range(1, N_COL):
        pl.semaphore_signal(barrier, inc=1, device_id=(rho, lax.rem(col + i, N_COL)), device_id_type=MESH)
    for i in range(1, N_ROW):
        pl.semaphore_signal(barrier, inc=1, device_id=(lax.rem(rho + i, N_ROW), col), device_id_type=MESH)
    diagonals = ((-1, -1), (-1, 1), (1, -1), (1, 1))

    def exists(dr, dc):
        ok = None
        for at, step, size in ((rho, dr, N_ROW), (col, dc, N_COL)):
            if step:
                here = (at > 0) if step < 0 else (at < size - 1)
                ok = here if ok is None else jnp.logical_and(ok, here)
        return ok

    for dr, dc in diagonals:
        @pl.when(exists(dr, dc))
        def _():
            pl.semaphore_signal(barrier, inc=1, device_id=(rho + dr, col + dc), device_id_type=MESH)

    fetches = [
        pltpu.make_async_copy(far, near, in_sem.at[n])
        for n, (far, near) in enumerate((
            (cond_hbm, cond), (mask_hbm, mask), (gidx_hbm, gidx), (sidx_hbm, sidx), (scur_hbm, scur),
        ))
    ]
    for fetch in fetches:
        fetch.start()
    for fetch in fetches:
        fetch.wait()
    mwin[MARGIN : MARGIN + CR, 0:CC] = cond[...] * mask[...].astype(F32)

    near = ((-1, 0, 0), (1, 0, 0), (0, -1, 0), (0, 1, 0))
    far = ((-1, 0, 1), (1, 0, 1)) + tuple((dr, dc, 1) for dr, dc in diagonals)
    around = near + far

    def land(dr, dc, part):
        if dc == 0:
            first = (8 - 8 * part) if dr < 0 else MARGIN + CR + 8 * part
            return mwin.at[pl.ds(first, 8), pl.ds(0, CC)]
        rows = {-1: pl.ds(0, MARGIN), 0: pl.ds(MARGIN, CR), 1: pl.ds(MARGIN + CR, MARGIN)}[dr]
        return (side_r if dc > 0 else side_l).at[rows, :]

    def take(dr, dc, part):
        if dc == 0:
            first = (MARGIN + 8 * part) if dr < 0 else MARGIN + CR - 8 - 8 * part
            return mwin.at[pl.ds(first, 8), pl.ds(0, CC)]
        rows = {-1: pl.ds(MARGIN, MARGIN), 0: pl.ds(MARGIN, CR), 1: pl.ds(CR, MARGIN)}[dr]
        return mwin.at[rows, pl.ds(0, 128) if dc < 0 else pl.ds(CC - 128, 128)]

    for dr, dc, part in around:
        @pl.when(jnp.logical_not(exists(dr, dc)))
        def _():
            ref = land(dr, dc, part)
            ref[...] = jnp.zeros(ref.shape, F32)

    def halo_start(n):
        dr, dc, part = around[n]
        m = around.index((-dr, -dc, part))
        @pl.when(exists(dr, dc))
        def _():
            pltpu.make_async_remote_copy(
                src_ref=take(dr, dc, part), dst_ref=land(-dr, -dc, part),
                send_sem=halo_send.at[n], recv_sem=halo_recv.at[m],
                device_id=(rho + dr, col + dc), device_id_type=MESH,
            ).start()

    def halo_wait(n):
        dr, dc, part = around[n]
        @pl.when(exists(dr, dc))
        def _():
            pltpu.make_async_remote_copy(
                src_ref=take(dr, dc, part), dst_ref=land(dr, dc, part),
                send_sem=halo_send.at[n], recv_sem=halo_recv.at[n],
                device_id=(rho + dr, col + dc), device_id_type=MESH,
            ).wait()

    expected = N_COL - 1 + N_ROW - 1
    for dr, dc in diagonals:
        expected = expected + exists(dr, dc).astype(jnp.int32)
    pl.semaphore_wait(barrier, expected)

    for n in range(len(around)):
        halo_start(n)

    gflat = flat_row(gidx[...].astype(F32)).astype(jnp.int32)
    sflat = flat_row(sidx[...].astype(F32)).astype(jnp.int32)
    cflat = flat_row(scur[...])
    g_row, g_col = gflat // NC, gflat % NC
    s_row, s_col = sflat // NC, sflat % NC

    own_b = iota((NB, 256), 1) // 16 == iota((NB, 256), 0)
    g_rel = g_row - rho * CR + MARGIN
    s_rel = s_row - rho * CR + MARGIN
    c_hi = cflat.astype(BF16).astype(F32)
    c_mid = (cflat - c_hi).astype(BF16).astype(F32)
    c_lo = cflat - c_hi - c_mid

    def build(r, carry):
        g_hit = jnp.logical_and(own_b, g_rel == r)
        s_hit = jnp.logical_and(own_b, s_rel == r)
        lhs_g[r] = jnp.where(g_hit, 1.0, 0.0).astype(BF16)
        lhs_s[r, :, 0:256] = jnp.where(s_hit, c_hi, 0.0).astype(BF16)
        lhs_s[r, :, 256:512] = jnp.where(s_hit, c_mid, 0.0).astype(BF16)
        lhs_s[r, :, 512:768] = jnp.where(s_hit, c_lo, 0.0).astype(BF16)
        return carry

    lax.fori_loop(0, WR, build, 0, unroll=4)

    def place(column):
        rel = column - col * CC
        return jnp.where(rel >= 576, -1, jnp.where(rel >= 0, rel, jnp.where(rel >= -64, rel + WC, -1)))

    spot = 5 * (iota((WC, 256), 0) % 128) + iota((WC, 256), 0) // 128
    g_hot = jnp.where(place(g_col) == spot, 1.0, 0.0).astype(BF16)
    s_one = jnp.where(place(s_col) == spot, 1.0, 0.0).astype(BF16)
    s_hot = jnp.concatenate([s_one, s_one, s_one], axis=1)

    STEP = 32

    def spread(i, carry):
        rows = pl.ds(i * STEP, STEP)
        diag[rows] = lax.dot_general(
            lhs_g[rows].reshape(STEP * NB, 256), g_hot, NT, preferred_element_type=F32
        ).reshape(STEP, NB, WC)
        hsrc[rows] = lax.dot_general(
            lhs_s[rows].reshape(STEP * NB, 768), s_hot, NT, preferred_element_type=F32
        ).reshape(STEP, NB, WC)
        return carry

    lax.fori_loop(0, WR // STEP, spread, 0)

    a1 = jnp.where(g_col // CC == iota((8, 256), 0), 1.0, 0.0).astype(BF16)
    a2 = jnp.where(
        jnp.logical_and(
            g_row // CR == iota((256, 256), 0) // 16,
            iota((256, 256), 1) // 16 == iota((256, 256), 0) % 16,
        ), 1.0, 0.0).astype(BF16)
    shunt_total = lax.dot_general(a1, a2, NT, preferred_element_type=F32)

    mrow[3, MARGIN : MARGIN + CR, :] = jnp.where(
        interleave(jnp.concatenate([mwin[MARGIN : MARGIN + CR, 0:CC], jnp.zeros((CR, 128), F32)], axis=1)) > 0.0,
        1.0, 0.0,
    )
    wide_zero = jnp.zeros((NB, WC), F32)
    inflow_acc = lax.fori_loop(
        MARGIN, MARGIN + CR, lambda r, acc: acc + hsrc[r] * mrow[3, pl.ds(r, 1), :], wide_zero, unroll=4
    )

    def total(field):
        return jnp.sum(jnp.sum(field, axis=0, keepdims=True), axis=1, keepdims=True)

    slot = iota((NB, 128), 1) // 16
    own_slot = slot == lax.rem(rho, 8)
    same_b = iota((NB, 128), 1) % 16 == iota((NB, 128), 0)
    row_slot = iota((1, 128), 1) // 16 == lax.rem(rho, 8)

    def one_row(value):
        return jnp.where(row_slot, jnp.broadcast_to(value, (1, 128)), 0.0)

    def b_row(acc, where):
        value = jnp.sum(acc, axis=1, keepdims=True)
        return jnp.sum(jnp.where(jnp.logical_and(where, same_b), value, 0.0), axis=0, keepdims=True)

    own_col = at_col() < CC

    def fold(x):
        parts = tiles(jnp.where(own_col, x, 0.0))
        return parts[0] + parts[1] + ((parts[2] + parts[3]) + parts[4])

    inflow_row = b_row(fold(inflow_acc), own_slot)

    def put_natural(n, field, lo, hi, less=None):
        def step(r, carry):
            for half in range(2):
                sub = pl.ds(8 * half, 8)
                value = field[r + MARGIN, sub, :]
                if less is not None:
                    value = 81.0 * (value - less[8 * half : 8 * half + 8])
                nat[n, sub, r, :] = natural(tiles(value))
            return carry

        lax.fori_loop(lo, hi, step, 0, unroll=4)

    def ring(d):
        return min(d, 4 - d)

    slow, fast = rho // 4, lax.rem(rho, 4)
    row_steps = sorted(((a, b) for a in range(4) for b in range(4) if a or b), key=lambda t: -ring(t[0]) - ring(t[1]))
    row_peers = [lax.rem(slow + a, 4) * 4 + lax.rem(fast + b, 4) for a, b in row_steps]
    chip, core = col // 2, lax.rem(col, 2)
    col_steps = sorted(((a, b) for a in range(4) for b in range(2) if a or b), key=lambda t: (-ring(t[0]), -t[1]))
    col_peers = [lax.rem(chip + a, 4) * 2 + lax.rem(core + b, 2) for a, b in col_steps]

    def send_a(g, rows):
        ga = gas[g]
        ga[rho] = jnp.concatenate(rows, axis=0)
        for peer in row_peers:
            pltpu.make_async_remote_copy(
                src_ref=ga.at[rho], dst_ref=ga.at[rho], send_sem=ga_send.at[g], recv_sem=ga_recv.at[g],
                device_id=(peer, col), device_id_type=MESH,
            ).start()

    def send_b(g):
        ga, gb = gas[g], gbs[g]
        peers = pl.ds(0, N_ROW - 1)
        pltpu.make_async_remote_copy(
            src_ref=ga.at[peers], dst_ref=ga.at[peers], send_sem=ga_send.at[g], recv_sem=ga_recv.at[g],
            device_id=(lax.rem(rho + 1, N_ROW), col), device_id_type=MESH,
        ).wait()
        for h in range(2):
            acc = ga[8 * h]
            for i in range(1, 8):
                acc = acc + ga[8 * h + i]
            gb[col, h] = acc
        for peer in col_peers:
            pltpu.make_async_remote_copy(
                src_ref=gb.at[col], dst_ref=gb.at[col], send_sem=gb_send.at[g], recv_sem=gb_recv.at[g],
                device_id=(rho, peer), device_id_type=MESH,
            ).start()

    def wait_b(g):
        gb = gbs[g]
        peers = pl.ds(0, N_COL - 1)
        pltpu.make_async_remote_copy(
            src_ref=gb.at[peers], dst_ref=gb.at[peers], send_sem=gb_send.at[g], recv_sem=gb_recv.at[g],
            device_id=(rho, lax.rem(col + 1, N_COL)), device_id_type=MESH,
        ).wait()

    def coarse(g, k):
        gb = gbs[g]
        return jnp.concatenate([gb[:, 0, k, :], gb[:, 1, k, :]], axis=1)

    for n in range(len(near)):
        halo_wait(n)
    inner = slice(MARGIN, MARGIN + CR)
    lane = iota((WR, 128), 1)
    beside = jnp.where(lane[0:CR] < 64, side_r[inner, :], side_l[inner, :])
    m = jnp.concatenate([mwin[inner, 0:CC], beside], axis=1)

    def held_of(x):
        return jnp.where(x > 0.0, 1.0, 0.0)

    present = held_of(m)
    east = 0.5 * present * roll(present, -1) * (m + roll(m, -1))
    west = roll(east, 1)[:, 0:CC]
    east = east[:, 0:CC]
    m, present = m[:, 0:CC], present[:, 0:CC]
    m_s, m_n = mwin[MARGIN + 1 : MARGIN + CR + 1, 0:CC], mwin[MARGIN - 1 : MARGIN + CR - 1, 0:CC]
    south = 0.5 * present * held_of(m_s) * (m + m_s)
    north = 0.5 * held_of(m_n) * present * (m_n + m)
    base = east + west + south + north + LEAKAGE
    gap_total = total((((base - east) - west) - south) - north - LEAKAGE)
    east_total = jnp.sum(east[:, CC - 1 : CC], axis=0, keepdims=True)
    south_total = jnp.sum(south[CR - 1 : CR, :], axis=1, keepdims=True)
    send_a(0, [inflow_row, one_row(east_total), one_row(south_total), one_row(gap_total)])

    for n in range(len(near), len(around)):
        halo_wait(n)
    mwin[0:WR, CC:WC] = jnp.where(lane < 64, side_r[...], side_l[...])

    m = interleave(mwin[...])
    mrow[0] = m
    last = jnp.zeros((1, WC), F32)
    m_s = jnp.concatenate([mrow[0, 1:WR, :], last], axis=0)
    present = jnp.where(m > 0.0, 1.0, 0.0)
    present_s = jnp.where(m_s > 0.0, 1.0, 0.0)
    east = 0.5 * present * east_of(present) * (m + east_of(m))
    south = 0.5 * present * present_s * (m + m_s)
    west = west_of(east)
    mrow[0] = south
    north = jnp.concatenate([last, mrow[0, 0 : WR - 1, :]], axis=0)
    base = east + west + south + north + LEAKAGE
    mrow[1] = base
    mrow[2] = east
    mrow[3] = present
    at_r = iota((WR, WC), 0)
    at_c = jnp.broadcast_to(at_col(), (WR, WC))
    row_in = jnp.where(jnp.logical_and(at_r >= MARGIN, at_r < MARGIN + CR), 1.0, 0.0)
    row_in_s = jnp.where(jnp.logical_and(at_r >= MARGIN - 1, at_r < MARGIN + CR - 1), 1.0, 0.0)
    row_in_n = jnp.where(jnp.logical_and(at_r >= MARGIN + 1, at_r < MARGIN + CR + 1), 1.0, 0.0)
    col_in = jnp.where(at_c < CC, 1.0, 0.0)
    col_in_e = jnp.where(jnp.logical_or(at_c < CC - 1, at_c == WC - 1), 1.0, 0.0)
    col_in_w = jnp.where(jnp.logical_and(at_c >= 1, at_c <= CC), 1.0, 0.0)
    inside = row_in * col_in

    mrow[4] = (
        base * inside - east * (row_in * col_in_e) - west * (row_in * col_in_w)
        - south * (row_in_s * col_in) - north * (row_in_n * col_in)
    )
    mrow[5] = inside

    def coeffs(r, inner):
        rows = pl.ds(r, 1)
        shunt = diag[r]
        d = shunt + mrow[1, rows, :]
        inverse = 2.0 / d
        here = hsrc[r] * mrow[3, rows, :]
        winv3[r] = inverse
        v1[r] = (1.0 / 3.0) * inverse * here
        e_east[r] = jnp.broadcast_to(mrow[2, rows, :], (8, WC))
        e_south[r] = jnp.broadcast_to(mrow[0, rows, :], (8, WC))
        if inner:
            diag[r] = d
            hsrc[r] = here
            kappa[r] = mrow[4, rows, :] + shunt * mrow[5, rows, :]

    def coeffs_rim(i, carry):
        coeffs(1 + i, False)
        coeffs(MARGIN + CR + i, False)
        return carry

    def coeffs_block(i, carry):
        coeffs(MARGIN + 2 * i, True)
        coeffs(MARGIN + 2 * i + 1, True)
        return carry

    e_south[0] = jnp.broadcast_to(mrow[0, 0:1, :], (8, WC))
    lax.fori_loop(0, MARGIN - 1, coeffs_rim, 0)
    lax.fori_loop(0, CR // 2, coeffs_block, 0)
    for r in (MARGIN - 1, MARGIN + CR):
        kappa[r] = jnp.broadcast_to(mrow[4, r : r + 1, :], (NB, WC))

    def sweep(src, dst, width, extra=None, scale=None, image=None):
        rows = CR + 2 * width
        at_once = min(range(CHOICES[0], CHOICES[1]), key=lambda n: (-(-rows // n) * n, -n))
        count = -(-rows // at_once)
        lo = MARGIN - width - (count * at_once - rows) // 2

        def step(i, carry):
            r0 = lo + i * at_once
            for k in range(at_once):
                r = r0 + k
                e = tiles(e_east[r])
                south_here = tiles(e_south[r])
                south_north = tiles(e_south[r - 1])
                for half in range(2):
                    sub = pl.ds(8 * half, 8)
                    s = tiles(src[r, sub, :])
                    below = tiles(src[r + 1, sub, :])
                    above = tiles(src[r - 1, sub, :])
                    w3 = tiles(winv3[r, sub, :])
                    h = None if extra is None else tiles(extra[r, sub, :])
                    to_east = s[1:] + [roll(s[0], -1)]
                    flow = [e[j] * s[j] for j in range(4)]
                    to_west = [roll(e[4] * s[4], 1)] + flow
                    for j in range(5):
                        t = (e[j] * to_east[j] + to_west[j]) + (south_here[j] * below[j] + south_north[j] * above[j])
                        at = pl.ds(128 * j, 128)
                        if image is not None:
                            image[r, sub, at] = diag[r, sub, at] * s[j] - t
                        if dst is not None:
                            new = s[j] + w3[j] * t
                            if h is not None:
                                new = new + scale * h[j]
                            dst[r, sub, at] = new
            return carry

        lax.fori_loop(0, count, step, 0)

    def block_image(field):
        acc = lax.fori_loop(
            MARGIN - 1, MARGIN + CR + 1, lambda r, acc: acc + field[r] * kappa[r], wide_zero, unroll=2
        )
        parts = tiles(acc)
        return (parts[0] + parts[1]) + (parts[2] + parts[3]) + parts[4]

    def own_dots(*pairs):
        def step(r, accs):
            return tuple(acc + f[r] * g[r] for acc, (f, g) in zip(accs, pairs))

        accs = lax.fori_loop(MARGIN, MARGIN + CR, step, (wide_zero,) * len(pairs), unroll=4)
        return [fold(acc) for acc in accs]

    sweep(v1, s_a, 14, v1, 3.0)
    sweep(s_a, s_b, 13, v1, 9.0)
    sweep(s_b, s_a, 12, v1, 27.0)
    send_b(0)
    sweep(s_a, s_b, 11, v1, 81.0)
    ra = block_image(s_b) * (1.0 / 81.0)
    zero_row = jnp.zeros((1, 128), F32)
    send_a(1, [b_row(ra, own_slot), zero_row])
    ru = own_dots((s_b, hsrc))[0] * (1.0 / 81.0)

    put_natural(0, s_b, 0, EARLY)
    wait_b(0)
    f0 = coarse(0, 0)
    ec = coarse(0, 1)
    sc = coarse(0, 2)
    gap = coarse(0, 3)
    degree = LEAKAGE * CR * CC + shunt_total + ec + pltpu.roll(ec, 1, 0) + sc + roll(sc, 16)
    sub = iota((8, 256), 0)
    t = []
    for j in range(8):
        tj = jnp.where(sub == j, degree, 0.0)
        tj = jnp.where(sub == j - 1, -ec, tj)
        tj = jnp.where(sub == j + 1, -jnp.broadcast_to(ec[j : j + 1, :], (8, 256)), tj)
        t.append(tj)
    uvec = -sc
    lvec = roll(uvec, 16)
    x = mat_inv(t)
    for j in range(8):
        cfac[0, j] = x[j]
    ux = [uvec * x[j] for j in range(8)]
    lx = [lvec * x[j] for j in range(8)]
    p = [ux[j] * uvec[j : j + 1, :] for j in range(8)]
    q = [lx[j] * lvec[j : j + 1, :] for j in range(8)]
    w = [ux[j] * lvec[j : j + 1, :] for j in range(8)]
    wt = [lx[j] * uvec[j : j + 1, :] for j in range(8)]
    for level in range(1, 5):
        d = 16 << (level - 1)
        t = [t[j] - roll(p[j], d) - roll(q[j], -d) for j in range(8)]
        x = mat_inv(t)
        for j in range(8):
            cfac[level, j] = x[j]
        if level == 4:
            break
        low = [-roll(w[j], d) for j in range(8)]
        up = [-roll(wt[j], -d) for j in range(8)]
        low_t = [-roll(wt[j], d) for j in range(8)]
        up_t = [-roll(w[j], -d) for j in range(8)]
        for j in range(8):
            clow[level - 1, j] = low[j]
            cup[level - 1, j] = up[j]
        y = mat_mat(x, up)
        z = mat_mat(x, low)
        p = mat_mat(up_t, y)
        q = mat_mat(low_t, z)
        w = mat_mat(up_t, z)
        wt = mat_mat(low_t, y)

    def solve(f):
        h = mat_vec([cfac[0, j] for j in range(8)], f)
        f = f - lvec * roll(h, 16) - uvec * roll(h, -16)
        for level in range(1, 4):
            d = 16 << level
            h = mat_vec([cfac[level, j] for j in range(8)], f)
            f = f - mat_vec([clow[level - 1, j] for j in range(8)], roll(h, d))
            f = f - mat_vec([cup[level - 1, j] for j in range(8)], roll(h, -d))
        return mat_vec([cfac[4, j] for j in range(8)], f)

    wide_b = iota((NB, 256), 1) % 16 == iota((NB, 256), 0)

    def to_b(row):
        return jnp.sum(jnp.where(wide_b, row, 0.0), axis=1, keepdims=True)

    def dot_c(a, b):
        return to_b(jnp.sum(a * b, axis=0, keepdims=True))

    lane_c = jnp.broadcast_to(at_col(), (NB, WC))

    def around_field(y):
        fields = []
        lane_row = iota((8, 256), 1) // 16
        for dr in (-1, 0, 1):
            vals = []
            for dc in (0, 1, -1):
                hit = jnp.logical_and(lane_row == rho + dr, sub == col + dc)
                vals.append(to_b(jnp.sum(jnp.where(hit, y, 0.0), axis=0, keepdims=True)))
            fields.append(jnp.where(lane_c < CC, vals[0], jnp.where(lane_c < CC + 64, vals[1], vals[2])))
        return fields

    def combine(dst, src, fields, width, scale):
        spans = ((MARGIN - width, MARGIN), (MARGIN, MARGIN + CR), (MARGIN + CR, MARGIN + CR + width))
        for (lo, hi), field in zip(spans, fields):
            def step(r, carry):
                dst[r] = field + scale * src[r]
                return carry
            lax.fori_loop(lo, hi, step, 0, unroll=hi - lo if hi - lo < 16 else 4)

    y0 = solve(f0)
    combine(v0, s_b, around_field(y0), 11, 1.0 / 81.0)

    send_b(1)
    sweep(v0, s_a, 10, image=w0)
    sweep(s_a, s_b, 9)
    sweep(s_b, s_a, 8)
    sweep(s_a, s_b, 7)
    sweep(s_b, s_a, 6)
    ra0 = block_image(s_a) * (1.0 / 243.0)
    send_a(2, [b_row(ra0, own_slot), zero_row])
    (mu0,) = own_dots((v0, w0))
    wait_b(1)
    f1 = f0 + coarse(1, 0) + gap * y0
    g0 = solve(f1)
    combine(v1, s_a, around_field(g0), 6, -1.0 / 243.0)

    sweep(v1, s_b, 5, image=w1)
    sweep(s_b, s_a, 4)
    sweep(s_a, s_b, 3)
    sweep(s_b, s_a, 2)
    sweep(s_a, s_b, 1)
    mu1, mu2 = own_dots((v1, w0), (v1, w1))
    sweep(s_b, None, 0, image=s_a)
    send_b(2)
    bab, bw1 = own_dots((s_b, s_a), (s_b, w1))
    bab = bab * (1.0 / (243.0 * 243.0))
    bw1 = bw1 * (1.0 / 243.0)
    ra1 = block_image(s_b) * (1.0 / 243.0)
    moments = zero_row
    for n, acc in enumerate((ru, mu0, mu1, mu2, bw1, bab)):
        moments = moments + b_row(acc, slot == n)
    send_a(3, [b_row(ra1, own_slot), moments])
    own_block = jnp.logical_and(iota((8, 256), 1) // 16 == rho, sub == col)

    def own_value(y):
        return to_b(jnp.sum(jnp.where(own_block, y, 0.0), axis=0, keepdims=True))

    y0_own = own_value(y0)
    put_natural(1, v1, 0, CR)
    wait_b(2)
    f2 = f1 - coarse(2, 0) + gap * g0
    g1 = solve(f2)
    put_natural(2, s_b, 0, CR // 2)
    send_b(3)
    put_natural(2, s_b, CR // 2, CR)
    put_natural(0, v0, EARLY, CR, jnp.broadcast_to(y0_own, (NB, WC)))
    g1_own = own_value(g1)
    energy_y = dot_c(f0, y0)
    g1w1 = dot_c(g1, f2)
    g1gap = dot_c(g1, g1 * gap)
    wait_b(3)
    ra1_all = coarse(3, 0)
    g1ra1 = dot_c(g1, ra1_all)
    mom = coarse(3, 1)
    mom = jnp.sum(mom[:, 0:128] + mom[:, 128:256], axis=0, keepdims=True)

    def moment(n):
        return jnp.sum(jnp.where(jnp.logical_and(slot == n, same_b), mom, 0.0), axis=1, keepdims=True)

    energy = moment(0) + energy_y
    m0, m1, m2 = moment(1), moment(2), moment(3)
    m3 = g1w1 - moment(4)
    m4 = g1w1 + g1gap - 2.0 * g1ra1 + moment(5)
    r1 = m0 - energy
    r2 = m1 - r1

    def ratio(a, b, scale):
        ok = b > scale
        return jnp.where(ok, a / jnp.where(ok, b, 1.0), 0.0)

    l10 = m1 / m0
    l20 = m2 / m0
    d1 = m2 - l10 * m1
    e21 = m3 - l20 * m1
    l21 = ratio(e21, d1, 0.0)
    d2 = m4 - l20 * m2 - l21 * e21
    t1 = r1 - l10 * energy
    t2 = r2 - l20 * energy - l21 * t1
    c2 = ratio(t2, d2, 0.0)
    c1 = ratio(t1, d1, 0.0) - l21 * c2
    c0 = energy / m0 - l10 * c1 - l20 * c2
    shift = c0 * y0_own + c2 * g1_own
    for n, c in enumerate((c0 * (1.0 / 81.0), c1, c2 * (-1.0 / 243.0), shift)):
        coef[n] = jnp.broadcast_to(c, (NB, CC))

    def finish(b, carry):
        w = [coef[n, pl.ds(b, 1), :] for n in range(4)]
        out[b] = w[0] * nat[0, b] + w[1] * nat[1, b] + (w[2] * nat[2, b] + w[3])
        return carry

    lax.fori_loop(0, NB, finish, 0, unroll=2)


def shards(conductance, nodata_mask, source_index, source_current, ground_index):
    big = pltpu.VMEM((WR, NB, WC), F32)
    edge = pltpu.VMEM((WR, 8, WC), F32)
    scratch = [
        pltpu.VMEM((CR, CC), F32), pltpu.VMEM((CR, CC), jnp.int32), pltpu.VMEM((NB, 16), jnp.int32),
        pltpu.VMEM((NB, 16), F32), pltpu.VMEM((NB, 16), jnp.int32), pltpu.SemaphoreType.DMA((5,)),
        pltpu.VMEM((WR, WC), F32), pltpu.VMEM((WR, 128), F32), pltpu.VMEM((WR, 128), F32),
        big, big, big, edge, edge, big,
        big, big, big, big, big, big,
        pltpu.VMEM((WR, NB, 256), BF16), pltpu.VMEM((WR, NB, 768), BF16),
        pltpu.VMEM((5, 8, 8, 256), F32), pltpu.VMEM((3, 8, 8, 256), F32), pltpu.VMEM((3, 8, 8, 256), F32),
        pltpu.VMEM((6, WR, WC), F32),
    ]
    for q in (4, 2, 2, 2):
        scratch += [pltpu.VMEM((N_ROW, q, 128), F32), pltpu.VMEM((N_COL, 2, q, 128), F32)]
    scratch += [pltpu.VMEM((3, NB, CR, CC), F32), pltpu.VMEM((4, NB, CC), F32)]
    scratch += [pltpu.SemaphoreType.DMA((10,)), pltpu.SemaphoreType.DMA((10,))]
    scratch += [pltpu.SemaphoreType.DMA((4,)) for _ in range(4)]
    return pl.pallas_call(
        body,
        out_shape=pltpu.VMEM((NB, CR, CC), F32),
        in_specs=[pl.BlockSpec(memory_space=pltpu.HBM)] * 5,
        out_specs=pl.BlockSpec(memory_space=pltpu.VMEM),
        scratch_shapes=scratch,
        compiler_params=pltpu.CompilerParams(
            collective_id=0, has_side_effects=True, vmem_limit_bytes=56 * 1024 * 1024
        ),
    )(conductance, nodata_mask, source_index, source_current, ground_index)


def solution(mesh):
    return jax.shard_map(
        shards,
        mesh=mesh,
        in_specs=(P("row", "col"), P("row", "col"), P(), P(), P()),
        out_specs=P(None, "row", "col"),
        check_vma=False,
    )
```
